128 devices in a mesh: lon: 8 (over x, y_hi), lat: 4 (over z), tm: 4 (over y_lo, core).
Axes of the slice: x: 4, y: 4 (y_hi: 2, y_lo: 2; y = y_hi * 2 + y_lo), z: 4, core: 2. Of those that a mesh axis runs over, the one named last changes fastest.
Arguments:
- precip: float32 [128, 1024, 1024], P('tm', 'lat', 'lon'), may hold values from 0.02 to 8
- offset: float32 [128, 1024, 1024], P('tm', 'lat', 'lon'), may hold values from -3 to 3
- coefficients: float32 [32, 256, 256], P('tm', 'lat', 'lon'), may hold values from -2 to 2
- inverse_diag: float32 [32, 256, 256], P('tm', 'lat', 'lon'), may hold values from 0.02 to 0.2
Outputs:
- newton_step: float32 [32, 256, 256], P('tm', 'lat', 'lon')
- residual: float32 [32, 256, 256], P('tm', 'lat', 'lon')
The draws below stay inside these ranges and needn't reach their ends.
All inputs are finite; a program needn't handle non-finite values.
Results may differ from the reference program's by a relative error of at most 0.0003.
Values sent between devices are 32-bit elements; how exact they have to be, the bound alone decides.
No kernel may reach another device: no remote copies, remote signals or barrier semaphores. Data moves between devices by JAX's collectives and lax.ppermute only.
A program may use at most 64 MiB of HBM per device.

```python
import math
import jax
import jax.numpy as jnp
from jax import lax

NT = 128
NLAT = 1024
NLON = 1024
KT = 32
KLAT = 256
KLON = 256


def shard_levels(own_key, shape, split, low, top_value):
    level = 1.0
    for axis_at, shards_of in split:
        heights = jax.random.uniform(jax.random.fold_in(jax.random.fold_in(own_key, 6), axis_at), (shards_of,), jnp.float32, low / len(split), top_value / len(split))
        level = level * jnp.repeat(jnp.exp(heights), shape[axis_at] // shards_of).reshape((-1,) + (1,) * (len(shape) - 1 - axis_at))
    return level


def normal_values(stream_key, shape, deviation, limit, pieces=(), held_as=jnp.bfloat16):
    drawn = deviation * jax.random.normal(stream_key, shape, jnp.float32)
    if pieces:
        drawn = drawn * shard_levels(stream_key, shape, pieces, -0.22, 0.18)
    return jnp.clip(drawn, -limit, limit).astype(held_as)


def setup_inputs(seed: int = 0) -> dict:
    keys = jax.random.split(jax.random.key(seed), 5)
    precip = jnp.clip(jnp.exp(math.log(8.0) - 5.9914646 * jax.random.uniform(keys[0], (NT, NLAT, NLON), jnp.float32) ** shard_levels(keys[0], (NT, NLAT, NLON), ((0, 4), (1, 4), (2, 8)), -0.2, 0.2)), 0.02, 8.0)
    offset = normal_values(keys[1], (NT, NLAT, NLON), 0.5, 3.0, ((0, 4), (1, 4), (2, 8)), jnp.float32)
    coefficients = normal_values(keys[2], (KT, KLAT, KLON), 0.3, 2.0, ((0, 4), (1, 4), (2, 8)), jnp.float32)
    inverse_diag = jnp.clip(jnp.exp(math.log(0.2) - 2.3025851 * jax.random.uniform(keys[3], (KT, KLAT, KLON), jnp.float32) ** shard_levels(keys[3], (KT, KLAT, KLON), ((0, 4), (1, 4), (2, 8)), -0.2, 0.2)), 0.02, 0.2)
    return dict(precip=precip, offset=offset, coefficients=coefficients, inverse_diag=inverse_diag)


tweedie_power = 1.6
smooth = 0.5
highest = lax.Precision.HIGHEST


def spline(offsets):
    distance = jnp.abs(offsets)
    near_part = (4.0 - 6.0 * distance * distance + 3.0 * distance * distance * distance) / 6.0
    far_part = jnp.maximum(2.0 - distance, 0.0) ** 3 / 6.0
    return jnp.where(distance < 1.0, near_part, far_part)


def spline_basis(cell_count, knot_count, cyclic):
    cell_pos = jnp.arange(cell_count, dtype=jnp.int32)[:, None]
    knot_pos = jnp.arange(knot_count, dtype=jnp.int32)[None, :]
    spread = cell_pos - 4 * knot_pos
    if cyclic:
        spread = jnp.mod(spread + cell_count // 2, cell_count) - cell_count // 2
        centred = spread.astype(jnp.float32) - 1.5
        return spline(centred / 4.0) + spline((centred - cell_count) / 4.0) + spline((centred + cell_count) / 4.0)
    return spline((spread.astype(jnp.float32) - 1.5) / 4.0)


def evaluate(vector, tables):
    time_tab, lat_tab, lon_tab = tables
    partial_value = jnp.einsum('tae,le->tal', vector, lon_tab, precision=highest)
    partial_value = jnp.einsum('tal,ba->tbl', partial_value, lat_tab, precision=highest)
    return jnp.einsum('tbl,st->sbl', partial_value, time_tab, precision=highest)


def adjoint(cell_values, tables):
    time_tab, lat_tab, lon_tab = tables
    partial_value = jnp.einsum('sbl,st->tbl', cell_values, time_tab, precision=highest)
    partial_value = jnp.einsum('tbl,ba->tal', partial_value, lat_tab, precision=highest)
    return jnp.einsum('tal,le->tae', partial_value, lon_tab, precision=highest)


def penalty(vector):
    summed = 18.0 * vector
    for along in (0, 1):
        padded = jnp.pad(vector, [(2, 2) if which == along else (0, 0) for which in range(3)])
        length = vector.shape[along]
        for first_at, factor in ((0, 1.0), (1, -4.0), (3, -4.0), (4, 1.0)):
            summed = summed + factor * lax.slice_in_dim(padded, first_at, first_at + length, axis=along)
    for moved, factor in ((2, 1.0), (1, -4.0), (-1, -4.0), (-2, 1.0)):
        summed = summed + factor * jnp.roll(vector, moved, axis=2)
    return smooth * summed


def reference(precip, offset, coefficients, inverse_diag):
    tables = (spline_basis(NT, KT, False), spline_basis(NLAT, KLAT, False), spline_basis(NLON, KLON, True))
    lat_index = jnp.arange(NLAT, dtype=jnp.float32)
    area_weight = jnp.cos((90.0 - (lat_index + 0.5) * 180.0 / NLAT) * (jnp.pi / 180.0))[None, :, None]
    linear = offset + evaluate(coefficients, tables)
    tilted = jnp.exp((1.0 - tweedie_power) * linear)
    mean_rate = jnp.exp(linear)
    weight = area_weight * mean_rate * tilted
    gradient = adjoint(area_weight * (mean_rate - precip) * tilted, tables) + penalty(coefficients)
    residual = -gradient
    scaled = inverse_diag * residual
    direction = scaled
    precond_norm = jnp.sum(residual * scaled)
    newton_step = jnp.zeros_like(coefficients)
    for sweep in range(2):
        image = adjoint(weight * evaluate(direction, tables), tables) + penalty(direction)
        step_size = precond_norm / jnp.sum(direction * image)
        newton_step = newton_step + step_size * direction
        residual = residual - step_size * image
        if sweep == 0:
            scaled = inverse_diag * residual
            next_norm = jnp.sum(residual * scaled)
            direction = scaled + (next_norm / precond_norm) * direction
            precond_norm = next_norm
    return newton_step, residual
```

```python
import jax
import jax.numpy as jnp
from jax import lax
from jax.sharding import PartitionSpec as P

SPLIT = ("tm", "lat", "lon")
tweedie_power = 1.6
smooth = 0.5
highest = lax.Precision.HIGHEST


def spline(offsets):
    distance = jnp.abs(offsets)
    near_part = (4.0 - 6.0 * distance * distance + 3.0 * distance * distance * distance) / 6.0
    far_part = jnp.maximum(2.0 - distance, 0.0) ** 3 / 6.0
    return jnp.where(distance < 1.0, near_part, far_part)


def synth_table(cell_count, knot_count):
    cell_pos = jnp.arange(cell_count, dtype=jnp.float32)[:, None]
    knot_pos = jnp.arange(knot_count + 4, dtype=jnp.float32)[None, :] - 2.0
    return spline((cell_pos - 4.0 * knot_pos - 1.5) / 4.0)


def matchings(count):
    first = [(i, i ^ 1) for i in range(count)]
    second = [(i, ((i + 1) ^ 1) - 1) for i in range(count)]
    return first, [(i, j % count) for i, j in second]


def swap_sides(to_left, to_right, axis):
    first, second = matchings(lax.axis_size(axis))
    odd = lax.axis_index(axis) % 2 == 1
    got_first = lax.ppermute(jnp.where(odd, to_left, to_right), axis, first)
    got_second = lax.ppermute(jnp.where(odd, to_right, to_left), axis, second)
    return jnp.where(odd, got_first, got_second), jnp.where(odd, got_second, got_first)


def inside(axis):
    index = lax.axis_index(axis)
    if axis == "lon":
        return 1.0, 1.0
    return (index > 0).astype(jnp.float32), (index < lax.axis_size(axis) - 1).astype(jnp.float32)


def cut(values, dim, start, stop):
    return lax.slice_in_dim(values, start, stop, axis=dim)


def expand(values):
    for dim, axis in ((1, "tm"), (2, "lat"), (3, "lon")):
        count = values.shape[dim]
        left, right = swap_sides(cut(values, dim, 0, 2), cut(values, dim, count - 2, count), axis)
        has_left, has_right = inside(axis)
        values = jnp.concatenate([left * has_left, values, right * has_right], axis=dim)
    return values


def merge(partial_sums):
    for dim, axis in ((0, "tm"), (1, "lat"), (2, "lon")):
        size = partial_sums.shape[dim]
        head, tail = cut(partial_sums, dim, 0, 4), cut(partial_sums, dim, size - 4, size)
        left, right = swap_sides(head, tail, axis)
        has_left, has_right = inside(axis)
        partial_sums = jnp.concatenate(
            [head + left * has_left, cut(partial_sums, dim, 4, size - 4), tail + right * has_right], axis=dim
        )
    return partial_sums


def evaluate(padded, tables):
    time_tab, lat_tab, lon_tab = tables
    partial_value = jnp.einsum("tae,le->tal", padded, lon_tab, precision=highest)
    partial_value = jnp.einsum("tal,ba->tbl", partial_value, lat_tab, precision=highest)
    return jnp.einsum("tbl,st->sbl", partial_value, time_tab, precision=highest)


def adjoint(cell_values, tables):
    time_tab, lat_tab, lon_tab = tables
    partial_value = jnp.einsum("sbl,st->tbl", cell_values, time_tab, precision=highest)
    partial_value = jnp.einsum("tbl,ba->tal", partial_value, lat_tab, precision=highest)
    return jnp.einsum("tal,le->tae", partial_value, lon_tab, precision=highest)


def penalty(padded):
    summed = jnp.zeros_like(padded)
    own = padded[2:-2, 2:-2, 2:-2]
    for dim, axis in ((0, "tm"), (1, "lat"), (2, "lon")):
        lines = padded[tuple(slice(None) if d == dim else slice(2, -2) for d in range(3))]
        size = lines.shape[dim]
        second = (
            cut(lines, dim, 0, size - 2) - 2.0 * cut(lines, dim, 1, size - 1) + cut(lines, dim, 2, size)
        )
        has_left, has_right = inside(axis)
        place = jnp.arange(size - 2).reshape([-1 if d == dim else 1 for d in range(3)])
        second = second * jnp.where(place == 0, 1.0 - has_left, jnp.where(place == size - 3, 1.0 - has_right, 1.0))
        spread = jnp.pad(second, [(2, 2) if d == dim else (0, 0) for d in range(3)])
        line_part = cut(spread, dim, 0, size) - 2.0 * cut(spread, dim, 1, size + 1) + cut(spread, dim, 2, size + 2)
        summed = summed + jnp.pad(line_part, [(0, 0) if d == dim else (2, 2) for d in range(3)])
    return smooth * summed


def all_sum(values):
    for axis, distances in (("tm", (1, 2, 3)), ("lat", (1, 2, 3)), ("lon", (2, 4, 6)), ("lon", (1,))):
        count = lax.axis_size(axis)
        values = values + sum(lax.ppermute(values, axis, [(i, i ^ d) for i in range(count)]) for d in distances)
    return values


def core(padded):
    return padded[2:-2, 2:-2, 2:-2]


def per_device(precip, offset, coefficients, inverse_diag):
    counts = coefficients.shape
    tables = tuple(synth_table(cells, knots) for cells, knots in zip(precip.shape, counts))
    lat_cells = precip.shape[1]
    lat_total = lat_cells * lax.axis_size("lat")
    lat_index = (lax.axis_index("lat") * lat_cells + jnp.arange(lat_cells, dtype=jnp.int32)).astype(jnp.float32)
    area_weight = jnp.cos((90.0 - (lat_index + 0.5) * 180.0 / lat_total) * (jnp.pi / 180.0))[None, :, None]

    both = expand(jnp.stack([coefficients, inverse_diag]))
    padded, diag = both[0], both[1]
    linear = offset + evaluate(padded, tables)
    rate = jnp.exp((2.0 - tweedie_power) * linear)
    weight = area_weight * rate
    slope = weight - area_weight * precip * jnp.exp((1.0 - tweedie_power) * linear)
    residual = -merge(adjoint(slope, tables) + penalty(padded))
    direction = diag * residual
    image_part = adjoint(weight * evaluate(direction, tables), tables) + penalty(direction)
    norm, curvature = all_sum(jnp.stack([jnp.sum(core(residual * direction)), jnp.sum(direction * image_part)]))
    image = merge(image_part)
    step_size = norm / curvature
    residual_next = residual - step_size * image
    scaled = diag * residual_next
    scaled_part = adjoint(weight * evaluate(scaled, tables), tables) + penalty(scaled)
    next_norm, curvature = all_sum(jnp.stack([jnp.sum(core(residual_next * scaled)), jnp.sum(scaled * scaled_part)]))
    scaled_image = core(merge(scaled_part))
    ratio = next_norm / norm
    step_next = next_norm / (curvature - ratio * next_norm / step_size)
    direction_own = core(direction)
    newton_step = step_size * direction_own + step_next * (core(scaled) + ratio * direction_own)
    last = core(residual_next) - step_next * (scaled_image + ratio * core(image))
    return newton_step, last


def solution(mesh):
    return jax.shard_map(
        per_device, mesh=mesh, in_specs=(P(*SPLIT),) * 4, out_specs=(P(*SPLIT),) * 2, check_vma=False
    )
```

```python
import functools

import jax
import jax.numpy as jnp
import numpy as np
from jax import lax
from jax.experimental import pallas as pl
from jax.experimental.pallas import tpu as pltpu
from jax.sharding import PartitionSpec as P

SPLIT = ("tm", "lat", "lon")
tweedie_power = 1.6
smooth = 0.5

ROWS, LANES, SEG, LAT_OWN, LON_OWN, T_OWN = 80, 512, 40, 64, 32, 8
HOURS, LAT_CELLS, LON_CELLS, BLOCK = 32, 256, 128, 128
STEPS = LAT_CELLS // BLOCK


def spline(offsets):
    distance = np.abs(offsets)
    near_part = (4.0 - 6.0 * distance**2 + 3.0 * distance**3) / 6.0
    far_part = np.maximum(2.0 - distance, 0.0) ** 3 / 6.0
    return np.where(distance < 1.0, near_part, far_part)


def table(cell_count, knot_count):
    cell_pos = np.arange(cell_count, dtype=np.float64)[:, None]
    knot_pos = np.arange(knot_count + 4, dtype=np.float64)[None, :] - 2.0
    return spline((cell_pos - 4.0 * knot_pos - 1.5) / 4.0)


def halves(values):
    values = jnp.asarray(values, jnp.float32)
    high = values.astype(jnp.bfloat16)
    return high, (values - high.astype(jnp.float32)).astype(jnp.bfloat16)


def tables():
    lat = np.zeros((LAT_CELLS, ROWS))
    lat[:, : LAT_OWN + 4] = table(LAT_CELLS, LAT_OWN)
    high, low = halves(lat)
    lat_up = jnp.concatenate([high, low, high], axis=1)
    high, low = (part.T.reshape(ROWS, STEPS, BLOCK).transpose(1, 0, 2) for part in (high, low))
    lat_down = jnp.concatenate([high, low, high], axis=2)
    lon = np.zeros((128, 3 * LON_CELLS))
    for r in range(3):
        lon[r * SEG : r * SEG + LON_OWN + 4, r * LON_CELLS : (r + 1) * LON_CELLS] = table(LON_CELLS, LON_OWN).T
    high, low = halves(lon)
    lon_up = jnp.concatenate([high, high, low], axis=0)
    lon_down = jnp.concatenate([high.T, low.T], axis=1)
    return lat_up, lat_down, lon_up, lon_down


def hour_factors():
    near, far = ([float(spline(np.float64(x))) for x in xs] for xs in ((0.125, 0.875, 0.375, 0.625), (1.125, 1.875, 1.375, 1.625)))
    outer = ((far[0] + far[1]) / 2, (far[0] - far[1]) / 2, (far[2] + far[3]) / 2, (far[2] - far[3]) / 2)
    inner = ((near[0] + near[1]) / 2, (near[0] - near[1]) / 2, (near[2] + near[3]) / 2, (near[2] - near[3]) / 2)
    return outer, inner


class Place:
    def __init__(self):
        index = {axis: lax.axis_index(axis) for axis in SPLIT}
        self.odd = {axis: index[axis] % 2 == 1 for axis in SPLIT}
        self.left = {axis: jnp.where(index[axis] > 0, 1.0, 0.0) for axis in SPLIT}
        self.right = {axis: jnp.where(index[axis] < lax.axis_size(axis) - 1, 1.0, 0.0) for axis in SPLIT}

    def messages(self, axis, to_left, to_right):
        return jnp.where(self.odd[axis], to_left, to_right), jnp.where(self.odd[axis], to_right, to_left)

    def received(self, axis, first, second):
        left, right = jnp.where(self.odd[axis], first, second), jnp.where(self.odd[axis], second, first)
        return (left, right) if axis == "lon" else (left * self.left[axis], right * self.right[axis])


def split(values):
    high = values.astype(jnp.bfloat16)
    return high, (values - high.astype(jnp.float32)).astype(jnp.bfloat16)


def dot(left, right):
    return jnp.dot(left, right, preferred_element_type=jnp.float32)


def lane_places():
    lane = lax.broadcasted_iota(jnp.int32, (ROWS, 128), 1)
    r = (lane >= SEG).astype(jnp.int32) + (lane >= 2 * SEG).astype(jnp.int32)
    return r, lane - SEG * r, lax.broadcasted_iota(jnp.int32, (ROWS, 128), 0)


def within(place, count):
    return (place >= 2) & (place < count + 2)


def group(values, g):
    return values[:, g * 128 : (g + 1) * 128]


def penalty(values, place):
    r, lon, row = lane_places()
    own_row, own_lon = within(row, LAT_OWN), within(lon, LON_OWN)
    row_share = jnp.where(
        own_row, 1.0, jnp.where(row == 1, 1.0 - place.left["lat"], jnp.where(row == LAT_OWN + 2, 1.0 - place.right["lat"], 0.0))
    )
    parts = [group(values, g) for g in range(4)]

    def along_t(v):
        before = [pltpu.roll(v[3], SEG, 1), v[0], v[1], v[2]]
        after = [v[1], v[2], v[3], pltpu.roll(v[0], 128 - SEG, 1)]
        return [b - 2.0 * m + a for b, m, a in zip(before, v, after)]

    t_second = along_t(parts)
    t_shared = []
    summed = []
    for g in range(4):
        t = 4 * r + g
        own_t = within(t, T_OWN)
        share = jnp.where(own_t, 1.0, jnp.where(t == 1, 1.0 - place.left["tm"], jnp.where(t == T_OWN + 2, 1.0 - place.right["tm"], 0.0)))
        t_shared.append(jnp.where(own_row & own_lon, share, 0.0) * t_second[g])
        v = parts[g]
        second = pltpu.roll(v, 1, 0) - 2.0 * v + pltpu.roll(v, ROWS - 1, 0)
        second = jnp.where(own_t & own_lon, row_share, 0.0) * second
        total = pltpu.roll(second, 1, 0) - 2.0 * second + pltpu.roll(second, ROWS - 1, 0)
        second = pltpu.roll(v, 1, 1) - 2.0 * v + pltpu.roll(v, 127, 1)
        second = jnp.where(own_t & own_lon & own_row, second, 0.0)
        summed.append(total + pltpu.roll(second, 1, 1) - 2.0 * second + pltpu.roll(second, 127, 1))
    return [smooth * (a + b) for a, b in zip(summed, along_t(t_shared))]


def lane_sum(parts):
    return jnp.sum(parts[0] + parts[1] + parts[2] + parts[3], axis=0, keepdims=True)


def own_lane_sum(values):
    r, lon, row = lane_places()
    inside = within(row, LAT_OWN) & within(lon, LON_OWN)
    return lane_sum([jnp.where(inside & within(4 * r + g, T_OWN), group(values, g), 0.0) for g in range(4)])


def merge_rows(values, got_first, got_second, place):
    keep = lax.broadcasted_iota(jnp.int32, (8, LANES), 0) < 4
    left, right = place.received("lat", got_first, got_second)
    return jnp.concatenate(
        [
            values[0:8] + jnp.where(keep, left, 0.0),
            values[8:64],
            values[64:72] + jnp.where(keep, right, 0.0),
            values[72:80],
        ],
        axis=0,
    )


def cell_block(block, vec_parts, w_of, lat_up, lat_down, lon_up, lon_down, up, down, before_cells):
    outer, inner = hour_factors()
    expanded = dot(lat_up[block * BLOCK : (block + 1) * BLOCK], vec_parts)
    high, low = split(jnp.concatenate([group(expanded, g) for g in range(4)], axis=0))
    up[...] = dot(jnp.concatenate([high, low, high], axis=1), lon_up[...])

    def tile(i, carry):
        start = pl.multiple_of(i * 8, 8)
        rows = pl.ds(pl.multiple_of(block * BLOCK + start, 8), 8)

        def knot(t):
            return up[pl.ds((t % 4) * BLOCK + start, 8), (t // 4) * 128 : (t // 4 + 1) * 128]

        back = [None] * 12

        def add(t, value):
            back[t] = value if back[t] is None else back[t] + value

        x = [knot(0), knot(1), knot(2), None]
        for j in range(9):
            x[3] = knot(j + 3)
            edge_sum, edge_diff, mid_sum, mid_diff = x[0] + x[3], x[0] - x[3], x[1] + x[2], x[1] - x[2]
            sides = []
            for pair, (late, early) in enumerate(((2, 1), (3, 0))):
                even = outer[2 * pair] * edge_sum + inner[2 * pair] * mid_sum
                uneven = outer[2 * pair + 1] * edge_diff + inner[2 * pair + 1] * mid_diff
                below = w_of(4 * (j - 1) + late, rows, even + uneven) if j > 0 else None
                above = w_of(4 * j + early, rows, even - uneven) if j < 8 else None
                if below is None:
                    sides.append((above, -above))
                elif above is None:
                    sides.append((below, below))
                else:
                    sides.append((below + above, below - above))
            (both0, differ0), (both1, differ1) = sides
            edge_even, edge_odd = outer[0] * both0 + outer[2] * both1, outer[1] * differ0 + outer[3] * differ1
            mid_even, mid_odd = inner[0] * both0 + inner[2] * both1, inner[1] * differ0 + inner[3] * differ1
            add(j, edge_even + edge_odd)
            add(j + 1, mid_even + mid_odd)
            add(j + 2, mid_even - mid_odd)
            add(j + 3, edge_even - edge_odd)
            for t in (j,) if j < 8 else (8, 9, 10, 11):
                down[pl.ds((t % 4) * BLOCK + start, 8), (t // 4) * 128 : (t // 4 + 1) * 128] = back[t]
            x = [x[1], x[2], x[3], None]
        return carry

    before_cells(block)
    lax.fori_loop(0, BLOCK // 8, tile, 0)
    high, low = split(down[...])
    both = dot(high, lon_down[...])
    narrow = both[:, :128] + both[:, 128:] + dot(low, lon_down[:, :128])
    narrow = jnp.concatenate([narrow[g * BLOCK : (g + 1) * BLOCK] for g in range(4)], axis=1)
    high, low = split(narrow)
    return dot(lat_down[block], jnp.concatenate([high, high, low], axis=0))


def apply_cells(values, w_of, place, lat_up, lat_down, lon_up, lon_down, up, down, before_cells=lambda block: None):
    high, low = split(values)
    parts = jnp.concatenate([high, high, low], axis=0)
    total = 0.0
    for block in range(STEPS):
        total = total + cell_block(block, parts, w_of, lat_up, lat_down, lon_up, lon_down, up, down, before_cells)
    extra = penalty(values, place)
    sums = [group(total, g) + extra[g] for g in range(4)]
    turned = [jnp.concatenate([part, jnp.zeros((128 - ROWS, 128), jnp.float32)], axis=0).T for part in sums]
    return sums, [[turned[g][r * SEG : (r + 1) * SEG] for g in range(4)] for r in range(3)]


def write_ends(segs, place, tiles, first, second):
    lower = lax.broadcasted_iota(jnp.int32, (8, 128), 0) < 4
    for r in range(3):
        for g in range(4):
            tiles[r, g] = segs[r][g]
        for h in range(2):
            packed = [
                jnp.where(lower, segs[r][2 * h][at : at + 8], pltpu.roll(segs[r][2 * h + 1][at : at + 8], 4, 0))
                for at in (0, 32)
            ]
            first[r, h], second[r, h] = place.messages("lon", *packed)


def start_kernel(both, got_first, got_second, area, offset_far, precip_far, lat_up, lat_down, lon_up, lon_down,
                 weight, diag, tiles, first, second, offset, precip, up, down, arrived):
    place = Place()
    copies = []
    for block in range(STEPS):
        rows = slice(block * BLOCK, (block + 1) * BLOCK)
        for source, target in ((offset_far, offset), (precip_far, precip)):
            at = arrived.at[len(copies)]
            copies.append(pltpu.make_async_copy(source.at[:, rows, :], target.at[:, rows, :], at))
    for copy in copies:
        copy.start()

    row = lax.broadcasted_iota(jnp.int32, (8, LANES), 0)
    left, right = place.received("lat", got_first[...], got_second[...])

    def with_halo(own, left, right):
        head, tail = own[0:8] + jnp.where(row < 2, left, 0.0), own[64:72] + jnp.where((row >= 2) & (row < 4), right, 0.0)
        return jnp.concatenate([head, own[8:64], tail, own[72:80]], axis=0)

    values = with_halo(both[0], left, right)
    diag[...] = with_halo(both[1], pltpu.roll(left, 6, 0), pltpu.roll(right, 6, 0))

    def w_of(hour, rows, value):
        linear = offset[hour, rows, :] + value
        here = area[rows, :]
        w = here * jnp.exp((2.0 - tweedie_power) * linear)
        weight[hour, rows, :] = w
        return w - here * precip[hour, rows, :] * jnp.exp((1.0 - tweedie_power) * linear)

    def before_cells(block):
        for copy in copies[2 * block : 2 * block + 2]:
            copy.wait()

    _, segs = apply_cells(values, w_of, place, lat_up, lat_down, lon_up, lon_down, up, down, before_cells)
    write_ends(segs, place, tiles, first, second)


def hessian_kernel(partial_rows, got_first, got_second, diag, weight, lat_up, lat_down, lon_up, lon_down, *refs, again):
    if again:
        before, residual, scaled, tiles, slots, up, down = refs
    else:
        residual, scaled, tiles, first, second, sums, up, down = refs
    place = Place()
    merged = merge_rows(partial_rows[...], got_first[...], got_second[...], place)
    here = merged if again else -merged
    residual[...] = here
    values = diag[...] * here
    scaled[...] = values

    def w_of(hour, rows, value):
        return weight[hour, rows, :] * value

    image, segs = apply_cells(values, w_of, place, lat_up, lat_down, lon_up, lon_down, up, down)
    lines = [own_lane_sum(here * values), lane_sum([image[g] * group(values, g) for g in range(4)])]
    if again:
        for r in range(3):
            for g in range(4):
                tiles[r, g] = segs[r][g]
        lines = jnp.concatenate([jnp.zeros((4, 128), jnp.float32), before[0:2], *lines], axis=0)
        write_slots(image, segs, lines, slots)
    else:
        write_ends(segs, place, tiles, first, second)
        sums[...] = jnp.concatenate(lines + [jnp.zeros((6, 128), jnp.float32)], axis=0)


def slot_at(lon_step, lat_step):
    lon_count, lat_count = lax.axis_size("lon"), lax.axis_size("lat")
    lon = lax.rem(lax.axis_index("lon") + (lon_count + lon_step), lon_count)
    return lon * lat_count + lax.rem(lax.axis_index("lat") + (lat_count + lat_step), lat_count)


def rolled(values, amount, axis):
    amount %= values.shape[axis]
    return pltpu.roll(values, amount, axis) if amount else values


def row_of(shape=(8, 128)):
    return lax.broadcasted_iota(jnp.int32, shape, 0)


def write_slots(sums, segs, lines, slots):
    row = row_of()
    low = lax.broadcasted_iota(jnp.int32, (8, 128), 1) < LAT_OWN
    for j in range(slots.shape[0]):
        slots[j, 0:8] = jnp.zeros((8, 128), jnp.float32)
        slots[j, 8:16] = lines
    for step, at, skip in ((-1, 0, 0), (1, 32, 2)):
        halves_of = [jnp.zeros((8, 128), jnp.float32), lines]
        for r in range(3):
            for h in range(2):
                index = 2 * r + h
                pair = jnp.where(
                    low, pltpu.roll(segs[r][2 * h][at : at + 8], 126, 1), pltpu.roll(segs[r][2 * h + 1][at : at + 8], 62, 1)
                )
                to = 2 * (index % 4)
                part = rolled(pair, to - skip, 0)
                halves_of[index // 4] = jnp.where((row >= to) & (row < to + 2), part, halves_of[index // 4])
        slot = slot_at(step, 0)
        slots[slot, 0:8] = halves_of[0]
        slots[slot, 8:16] = halves_of[1]
    for lat_step, at, skip in ((-1, 0, 0), (1, 64, 2)):
        content = jnp.zeros((8, 128), jnp.float32)
        for g in range(4):
            part = rolled(sums[g][at : at + 8], 2 * g - skip, 0)
            content = jnp.where((row >= 2 * g) & (row < 2 * g + 2), part, content)
        for lon_step in (-1, 0, 1):
            slots[slot_at(lon_step, lat_step), 0:8] = content


def collect_kernel(tiles, slots, merged, first, second, lines):
    place = Place()
    row = row_of()
    lane = lax.broadcasted_iota(jnp.int32, (8, 128), 1)
    own_lane = within(lane, LAT_OWN)
    r_of = (lane >= SEG).astype(jnp.int32) + (lane >= 2 * SEG).astype(jnp.int32)
    lon = lane - SEG * r_of
    sides = []
    for lat_step, share in ((-1, place.left["lat"]), (1, place.right["lat"])):
        before, same, after = (slots[slot_at(lon_step, lat_step), 0:8] for lon_step in (-1, 0, 1))
        side = jnp.where(within(lon, LON_OWN), same, 0.0)
        side = side + jnp.where(within(lon, 2), pltpu.roll(before, 128 - LON_OWN, 1), 0.0)
        side = side + jnp.where((lon >= LON_OWN) & (lon < LON_OWN + 2), pltpu.roll(after, LON_OWN, 1), 0.0)
        sides.append(side * share)
    blank = jnp.zeros((56, 128), jnp.float32)
    from_lat = []
    for g in range(4):
        head = jnp.where(within(row, 2), rolled(sides[0], 2 - 2 * g, 0), 0.0)
        tail = jnp.where(row < 2, rolled(sides[1], -2 * g, 0), 0.0)
        from_lat.append(jnp.concatenate([head, blank, tail, blank], axis=0).T)
    left = [slots[slot_at(-1, 0), at : at + 8] for at in (0, 8)]
    right = [slots[slot_at(1, 0), at : at + 8] for at in (0, 8)]
    for r in range(3):
        for g in range(4):
            index = 2 * r + g // 2
            shift = 66 if g % 2 else 2
            to = 2 * (index % 4)
            head = jnp.where(within(row, 2) & own_lane, pltpu.roll(rolled(left[index // 4], 2 - to, 0), shift, 1), 0.0)
            tail = jnp.where((row < 2) & own_lane, pltpu.roll(rolled(right[index // 4], -to, 0), shift, 1), 0.0)
            seg = tiles[r, g] + from_lat[g][r * SEG : (r + 1) * SEG]
            merged[r, g] = jnp.concatenate([seg[0:8] + head, seg[8:32], seg[32:40] + tail], axis=0)
    total = slots[0, 8:16]
    for j in range(1, slots.shape[0]):
        total = total + slots[j, 8:16]
    lines[...] = total
    low = lax.broadcasted_iota(jnp.int32, (SEG, 128), 1) < LAT_OWN

    def message(r, g):
        data = jnp.where(low, pltpu.roll(merged[r, g], 126, 1), pltpu.roll(merged[r, g + 1], 62, 1))
        return jnp.concatenate([data[:32], jnp.where(row < 4, data[32:], total)], axis=0)

    first[...], second[...] = place.messages("tm", message(0, 0), message(2, 2))


def join_kernel(tiles, got_first, got_second, joined, first, second):
    place = Place()
    lower = lax.broadcasted_iota(jnp.int32, (8, 128), 0) < 4
    for r in range(3):
        for g in range(4):
            left, right = place.received("lon", got_first[r, g // 2], got_second[r, g // 2])
            if g % 2:
                left, right = pltpu.roll(left, 4, 0), pltpu.roll(right, 4, 0)
            joined[r, g, 0:8] = tiles[r, g, 0:8] + jnp.where(lower, left, 0.0)
            joined[r, g, 8:32] = tiles[r, g, 8:32]
            joined[r, g, 32:40] = tiles[r, g, 32:40] + jnp.where(lower, right, 0.0)
    for g in range(4):
        first[g], second[g] = place.messages("tm", joined[0, g], joined[2, g])


def turned_rows(tiles, g, left=0.0, right=0.0):
    parts = [tiles[0, g] + left, tiles[1, g], tiles[2, g] + right, jnp.zeros((8, 128), jnp.float32)]
    return jnp.concatenate(parts, axis=0).T


def turn_kernel(tiles, got_first, got_second, rows, first, second):
    place = Place()
    for g in range(4):
        block = turned_rows(tiles, g, *place.received("tm", got_first[g], got_second[g]))
        lanes = slice(g * 128, (g + 1) * 128)
        rows[:, lanes] = block[:ROWS]
        first[:, lanes], second[:, lanes] = place.messages("lat", block[0:8], block[64:72])


def embed_kernel(coefficients, inverse_diag, tiles, first, second):
    place = Place()
    pair = lax.broadcasted_iota(jnp.int32, (8, 128), 0) // 2
    heads, tails = [None] * 4, [None] * 4
    for t in range(12):
        for k, values in enumerate((coefficients, inverse_diag)):
            if 2 <= t < T_OWN + 2:
                own = jnp.concatenate([values[t - 2], jnp.zeros((LON_OWN, 128 - LAT_OWN), jnp.float32)], axis=1)
                own = jnp.concatenate([own, jnp.zeros((SEG - LON_OWN, 128), jnp.float32)], axis=0)
                seg = pltpu.roll(pltpu.roll(own, 2, 0), 2, 1)
                at, tile = 2 * (t % 2) + k, (t - 2) // 2
                head, tail = rolled(seg[0:8], 2 * at - 2, 0), rolled(seg[32:40], 2 * at, 0)
                heads[tile] = head if at == 0 else jnp.where(pair == at, head, heads[tile])
                tails[tile] = tail if at == 0 else jnp.where(pair == at, tail, tails[tile])
            else:
                seg = jnp.zeros((SEG, 128), jnp.float32)
            tiles[k, t // 4, t % 4] = seg
    for tile in range(4):
        first[tile], second[tile] = place.messages("lon", heads[tile], tails[tile])


def embed_join_kernel(tiles, got_first, got_second, joined, first, second):
    place = Place()
    row = lax.broadcasted_iota(jnp.int32, (8, 128), 0)
    for k in range(2):
        for t in range(12):
            r, g = t // 4, t % 4
            if 2 <= t < T_OWN + 2:
                at, tile = 2 * (t % 2) + k, (t - 2) // 2
                left, right = place.received("lon", got_first[tile], got_second[tile])
                left, right = rolled(left, -2 * at, 0), rolled(right, 2 - 2 * at, 0)
                joined[k, r, g, 0:8] = tiles[k, r, g, 0:8] + jnp.where(row < 2, left, 0.0)
                joined[k, r, g, 8:32] = tiles[k, r, g, 8:32]
                joined[k, r, g, 32:40] = tiles[k, r, g, 32:40] + jnp.where((row >= 2) & (row < 4), right, 0.0)
            else:
                joined[k, r, g] = tiles[k, r, g]
    low = lax.broadcasted_iota(jnp.int32, (SEG, 128), 1) < LAT_OWN

    def beside(r, g):
        return jnp.where(low, pltpu.roll(joined[0, r, g], 126, 1), pltpu.roll(joined[1, r, g], 62, 1))

    for i in range(2):
        first[i], second[i] = place.messages("tm", beside(0, 2 + i), beside(2, i))


def embed_turn_kernel(tiles, got_first, got_second, rows, first, second):
    place = Place()
    lane = lax.broadcasted_iota(jnp.int32, (SEG, 128), 1)
    own = (lane >= 2) & (lane < LAT_OWN + 2)
    row = lax.broadcasted_iota(jnp.int32, (8, 128), 0)
    for g in range(4):
        lanes = slice(g * 128, (g + 1) * 128)
        left, right = place.received("tm", got_first[g % 2], got_second[g % 2])
        blocks = []
        for k in range(2):
            shift = 66 if k else 2
            if g < 2:
                block = turned_rows(tiles.at[k], g, left=jnp.where(own, pltpu.roll(left, shift, 1), 0.0))
            else:
                block = turned_rows(tiles.at[k], g, right=jnp.where(own, pltpu.roll(right, shift, 1), 0.0))
            rows[k, :, lanes] = block[:ROWS]
            blocks.append(block)
        head = jnp.where(row < 4, blocks[0][0:8], pltpu.roll(blocks[1][0:8], 2, 0))
        tail = jnp.where(row < 2, blocks[0][64:72], pltpu.roll(blocks[1][64:72], 2, 0))
        first[:, lanes], second[:, lanes] = place.messages("lat", head, tail)


def last_kernel(tiles, got_first, got_second, lines, got_lines, residual, scaled, image, image_scaled, step_out, residual_out):
    place = Place()
    left, right = place.received("tm", got_first[...], got_second[...])
    lane = lax.broadcasted_iota(jnp.int32, (SEG, 128), 1)
    own = within(lane, LAT_OWN)
    merged = []
    for g in range(4):
        side = right if g < 2 else left
        side = jnp.where(own, pltpu.roll(side, 66 if g % 2 else 2, 1), 0.0)
        block = turned_rows(tiles, g, right=side) if g < 2 else turned_rows(tiles, g, left=side)
        merged.append(block[:ROWS])
    merged = jnp.concatenate(merged, axis=1)
    total = lines[...] + got_lines[...] + got_first[32:40] + got_second[32:40]
    norm, curvature, image_norm, image_curvature = (jnp.sum(total[i : i + 1], axis=1, keepdims=True) for i in range(4, 8))
    step_size = norm / curvature
    next_norm = step_size * step_size * image_norm - norm
    ratio = next_norm / norm
    next_curvature = curvature - 2.0 * step_size * image_norm + step_size * step_size * image_curvature
    step_next = next_norm / (next_curvature - ratio * next_norm / step_size)
    direction = scaled[...] - step_size * image_scaled[...] + ratio * scaled[...]
    newton = step_size * scaled[...] + step_next * direction
    left_over = residual[...] - step_size * image[...] - step_next * (image[...] - step_size * merged + ratio * image[...])
    for values, out in ((newton, step_out), (left_over, residual_out)):
        for g in range(4):
            turned = jnp.concatenate([group(values, g), jnp.zeros((128 - ROWS, 128), jnp.float32)], axis=0).T
            turned = pltpu.roll(turned, 126, 1)
            for r in range(3):
                t = 4 * r + g - 2
                if 0 <= t < T_OWN:
                    out[t] = pltpu.roll(turned[r * SEG : (r + 1) * SEG], SEG - 2, 0)[:LON_OWN, :LAT_OWN]


def matchings(count):
    first = [(i, i ^ 1) for i in range(count)]
    return first, [(i, (((i + 1) ^ 1) - 1) % count) for i in range(count)]


def swap(first, second, axis):
    first_pairs, second_pairs = matchings(lax.axis_size(axis))
    return lax.ppermute(first, axis, first_pairs), lax.ppermute(second, axis, second_pairs)


def shaped(*shape):
    return jax.ShapeDtypeStruct(shape, jnp.float32)


def call(kernel, out_shape, name, *args, scratch=(), far=(), limit=24):
    vmem = pl.BlockSpec(memory_space=pltpu.VMEM)
    hbm = pl.BlockSpec(memory_space=pltpu.HBM)
    return pl.pallas_call(
        kernel,
        in_specs=[hbm if i in far else vmem for i in range(len(args))],
        out_specs=[vmem] * len(out_shape),
        out_shape=out_shape,
        scratch_shapes=scratch,
        compiler_params=pltpu.CompilerParams(vmem_limit_bytes=limit * 1024 * 1024),
        cost_estimate=pl.CostEstimate(flops=10**9, bytes_accessed=20 * 10**6, transcendentals=0),
        name=name,
    )(*args)


LON_MESSAGE, TM_MESSAGE, LAT_MESSAGE = (3, 2, 8, 128), (4, SEG, 128), (8, LANES)
TILES = (3, 4, SEG, 128)
VECTOR = (ROWS, LANES)
SCRATCH = [pltpu.VMEM((4 * BLOCK, 384), jnp.float32)] * 2
CELLS = (HOURS, LAT_CELLS, LON_CELLS)


def exchange(tiles, first, second):
    first, second = swap(first, second, "lon")
    tiles, first, second = call(
        join_kernel, (shaped(*TILES), shaped(*TM_MESSAGE), shaped(*TM_MESSAGE)), "join", tiles, first, second
    )
    first, second = swap(first, second, "tm")
    rows, first, second = call(
        turn_kernel, (shaped(*VECTOR), shaped(*LAT_MESSAGE), shaped(*LAT_MESSAGE)), "turn", tiles, first, second
    )
    return rows, *swap(first, second, "lat")


def fold_and_sum(tiles, slots, lines_shape):
    slots = lax.all_to_all(slots, ("lon", "lat"), 0, 0, tiled=True)
    message = shaped(SEG, 128)
    tiles, first, second, lines = call(
        collect_kernel, (shaped(*TILES), message, message, lines_shape), "collect", tiles, slots
    )
    first, second = swap(first, second, "tm")
    count = lax.axis_size("tm")
    return tiles, first, second, lines, lax.ppermute(lines, "tm", [(i, (i + 2) % count) for i in range(count)])


def expand(coefficients, inverse_diag):
    tiles, message = shaped(2, *TILES), shaped(4, 8, 128)
    tiles_here, first, second = call(
        embed_kernel, (tiles, message, message), "embed", coefficients, inverse_diag
    )
    first, second = swap(first, second, "lon")
    message = shaped(2, SEG, 128)
    tiles_here, first, second = call(embed_join_kernel, (tiles, message, message), "embed_join", tiles_here, first, second)
    first, second = swap(first, second, "tm")
    shapes = (shaped(2, *VECTOR), shaped(*LAT_MESSAGE), shaped(*LAT_MESSAGE))
    both, first, second = call(embed_turn_kernel, shapes, "embed_turn", tiles_here, first, second)
    return both, *swap(first, second, "lat")


def per_device(precip, offset, coefficients, inverse_diag):
    lat_total = LAT_CELLS * lax.axis_size("lat")
    lat_index = (lax.axis_index("lat") * LAT_CELLS + jnp.arange(LAT_CELLS, dtype=jnp.int32)).astype(jnp.float32)
    area = jnp.cos((90.0 - (lat_index + 0.5) * 180.0 / lat_total) * (jnp.pi / 180.0))
    area = jnp.broadcast_to(area[:, None], (LAT_CELLS, LON_CELLS))
    tabs = tables()
    ends = (shaped(*TILES), shaped(*LON_MESSAGE), shaped(*LON_MESSAGE))
    vector = shaped(*VECTOR)

    both = expand(coefficients.transpose(0, 2, 1), inverse_diag.transpose(0, 2, 1))
    weight, diag, tiles, first, second = call(
        start_kernel, (shaped(*CELLS), vector, *ends), "start", *both, area, offset, precip, *tabs,
        scratch=[pltpu.VMEM(CELLS, jnp.float32)] * 2 + SCRATCH + [pltpu.SemaphoreType.DMA((2 * STEPS,))],
        far=(4, 5), limit=47,
    )
    lines = shaped(8, 128)
    residual, scaled, tiles, first, second, sums = call(
        functools.partial(hessian_kernel, again=False), (vector, vector, *ends, lines), "hessian",
        *exchange(tiles, first, second), diag, weight, *tabs, scratch=SCRATCH,
    )
    slots = shaped(lax.axis_size("lon") * lax.axis_size("lat"), 16, 128)
    image, image_scaled, tiles, slots = call(
        functools.partial(hessian_kernel, again=True), (vector, vector, ends[0], slots), "hessian_again",
        *exchange(tiles, first, second), diag, weight, *tabs, sums, scratch=SCRATCH,
    )
    out = shaped(T_OWN, LON_OWN, LAT_OWN)
    outs = call(
        last_kernel, (out, out), "last", *fold_and_sum(tiles, slots, lines), residual, scaled, image, image_scaled
    )
    return tuple(v.transpose(0, 2, 1) for v in outs)


def solution(mesh):
    return jax.shard_map(
        per_device, mesh=mesh, in_specs=(P(*SPLIT),) * 4, out_specs=(P(*SPLIT),) * 2, check_vma=False
    )
```

```python
import functools

import jax
import jax.numpy as jnp
import numpy as np
from jax import lax
from jax.experimental import pallas as pl
from jax.experimental.pallas import tpu as pltpu
from jax.sharding import PartitionSpec as P

SPLIT = ("tm", "lat", "lon")
tweedie_power = 1.6
smooth = 0.5

ROWS, LANES, SEG, LAT_OWN, LON_OWN, T_OWN = 80, 512, 40, 64, 32, 8
HOURS, LAT_CELLS, LON_CELLS = 32, 256, 128
EDGE, CHUNK = 16, 32
MID_CELLS, EDGE_CELLS = LAT_CELLS - 2 * EDGE, 2 * EDGE
CHUNKS = MID_CELLS // CHUNK


def spline(offsets):
    distance = np.abs(offsets)
    near_part = (4.0 - 6.0 * distance**2 + 3.0 * distance**3) / 6.0
    far_part = np.maximum(2.0 - distance, 0.0) ** 3 / 6.0
    return np.where(distance < 1.0, near_part, far_part)


def table(cell_count, knot_count):
    cell_pos = np.arange(cell_count, dtype=np.float64)[:, None]
    knot_pos = np.arange(knot_count + 4, dtype=np.float64)[None, :] - 2.0
    return spline((cell_pos - 4.0 * knot_pos - 1.5) / 4.0)


def halves(values):
    values = jnp.asarray(values, jnp.float32)
    high = values.astype(jnp.bfloat16)
    return high, (values - high.astype(jnp.float32)).astype(jnp.bfloat16)


def middle(cells, axis=0):
    return lax.slice_in_dim(cells, EDGE, LAT_CELLS - EDGE, axis=axis)


def edges(cells, axis=0):
    ends = (lax.slice_in_dim(cells, at, at + EDGE, axis=axis) for at in (0, LAT_CELLS - EDGE))
    return jnp.concatenate(list(ends), axis=axis)


def tables():
    lat = np.zeros((LAT_CELLS, ROWS))
    lat[:, : LAT_OWN + 4] = table(LAT_CELLS, LAT_OWN)
    high, low = halves(lat)
    lat_tables = []
    for part in (middle, edges):
        up = jnp.concatenate([part(high), part(low), part(high)], axis=1)
        lat_tables += [up, jnp.concatenate([part(high).T, part(low).T, part(high).T], axis=1)]
    lon = np.zeros((128, 3 * LON_CELLS))
    for r in range(3):
        lon[r * SEG : r * SEG + LON_OWN + 4, r * LON_CELLS : (r + 1) * LON_CELLS] = table(LON_CELLS, LON_OWN).T
    high, low = halves(lon)
    lon_up = jnp.concatenate([high, high, low], axis=0)
    lon_down = jnp.concatenate([high.T, low.T], axis=1)
    return lat_tables[:2] + [lon_up, lon_down], lat_tables[2:] + [lon_up, lon_down]


def hour_factors():
    near, far = ([float(spline(np.float64(x))) for x in xs] for xs in ((0.125, 0.875, 0.375, 0.625), (1.125, 1.875, 1.375, 1.625)))
    outer = ((far[0] + far[1]) / 2, (far[0] - far[1]) / 2, (far[2] + far[3]) / 2, (far[2] - far[3]) / 2)
    inner = ((near[0] + near[1]) / 2, (near[0] - near[1]) / 2, (near[2] + near[3]) / 2, (near[2] - near[3]) / 2)
    return outer, inner


class Place:
    def __init__(self):
        index = {axis: lax.axis_index(axis) for axis in SPLIT}
        self.even = {axis: index[axis] % 2 == 0 for axis in SPLIT}
        self.left = {axis: jnp.where(index[axis] > 0, 1.0, 0.0) for axis in SPLIT}
        self.right = {axis: jnp.where(index[axis] < lax.axis_size(axis) - 1, 1.0, 0.0) for axis in SPLIT}

    def messages(self, axis, to_left, to_right):
        return jnp.where(self.even[axis], to_left, to_right), jnp.where(self.even[axis], to_right, to_left)

    def received(self, axis, first, second):
        left, right = jnp.where(self.even[axis], first, second), jnp.where(self.even[axis], second, first)
        return (left, right) if axis == "lon" else (left * self.left[axis], right * self.right[axis])


def split(values):
    high = values.astype(jnp.bfloat16)
    return high, (values - high.astype(jnp.float32)).astype(jnp.bfloat16)


def dot(left, right):
    return jnp.dot(left, right, preferred_element_type=jnp.float32)


def lane_places():
    lane = lax.broadcasted_iota(jnp.int32, (ROWS, 128), 1)
    r = (lane >= SEG).astype(jnp.int32) + (lane >= 2 * SEG).astype(jnp.int32)
    return r, lane - SEG * r, lax.broadcasted_iota(jnp.int32, (ROWS, 128), 0)


def within(place, count):
    return (place >= 2) & (place < count + 2)


def group(values, g):
    return values[:, g * 128 : (g + 1) * 128]


def penalty(values, place):
    r, lon, row = lane_places()
    own_row, own_lon = within(row, LAT_OWN), within(lon, LON_OWN)
    row_share = jnp.where(
        own_row, 1.0, jnp.where(row == 1, 1.0 - place.left["lat"], jnp.where(row == LAT_OWN + 2, 1.0 - place.right["lat"], 0.0))
    )
    parts = [group(values, g) for g in range(4)]

    def along_t(v):
        before = [pltpu.roll(v[3], SEG, 1), v[0], v[1], v[2]]
        after = [v[1], v[2], v[3], pltpu.roll(v[0], 128 - SEG, 1)]
        return [b - 2.0 * m + a for b, m, a in zip(before, v, after)]

    t_second = along_t(parts)
    t_shared = []
    summed = []
    for g in range(4):
        t = 4 * r + g
        own_t = within(t, T_OWN)
        share = jnp.where(own_t, 1.0, jnp.where(t == 1, 1.0 - place.left["tm"], jnp.where(t == T_OWN + 2, 1.0 - place.right["tm"], 0.0)))
        t_shared.append(jnp.where(own_row & own_lon, share, 0.0) * t_second[g])
        v = parts[g]
        second = pltpu.roll(v, 1, 0) - 2.0 * v + pltpu.roll(v, ROWS - 1, 0)
        second = jnp.where(own_t & own_lon, row_share, 0.0) * second
        total = pltpu.roll(second, 1, 0) - 2.0 * second + pltpu.roll(second, ROWS - 1, 0)
        second = pltpu.roll(v, 1, 1) - 2.0 * v + pltpu.roll(v, 127, 1)
        second = jnp.where(own_t & own_lon & own_row, second, 0.0)
        summed.append(total + pltpu.roll(second, 1, 1) - 2.0 * second + pltpu.roll(second, 127, 1))
    return [smooth * (a + b) for a, b in zip(summed, along_t(t_shared))]


def lane_sum(parts):
    return jnp.sum(parts[0] + parts[1] + parts[2] + parts[3], axis=0, keepdims=True)


def own_lane_sum(values):
    r, lon, row = lane_places()
    inside = within(row, LAT_OWN) & within(lon, LON_OWN)
    return lane_sum([jnp.where(inside & within(4 * r + g, T_OWN), group(values, g), 0.0) for g in range(4)])


def merge_rows(values, got_first, got_second, place):
    keep = lax.broadcasted_iota(jnp.int32, (8, LANES), 0) < 4
    left, right = place.received("lat", got_first, got_second)
    return jnp.concatenate(
        [
            values[0:8] + jnp.where(keep, left, 0.0),
            values[8:64],
            values[64:72] + jnp.where(keep, right, 0.0),
            values[72:80],
        ],
        axis=0,
    )


def apply_cells(values, w_of, lat_up, lat_down, lon_up, lon_down, up, down, before_chunk=None):
    outer, inner = hour_factors()
    cells = lat_up.shape[0]
    high, low = split(values)
    expanded = dot(lat_up[...], jnp.concatenate([high, high, low], axis=0))
    high, low = split(jnp.concatenate([group(expanded, g) for g in range(4)], axis=0))
    up[...] = dot(jnp.concatenate([high, low, high], axis=1), lon_up[...])

    def tile(i, carry):
        start = pl.multiple_of(i * 8, 8)
        rows = pl.ds(start, 8)

        def knot(t):
            return up[pl.ds((t % 4) * cells + start, 8), (t // 4) * 128 : (t // 4 + 1) * 128]

        back = [None] * 12

        def add(t, value):
            back[t] = value if back[t] is None else back[t] + value

        x = [knot(0), knot(1), knot(2), None]
        for j in range(9):
            x[3] = knot(j + 3)
            edge_sum, edge_diff, mid_sum, mid_diff = x[0] + x[3], x[0] - x[3], x[1] + x[2], x[1] - x[2]
            sides = []
            for pair, (late, early) in enumerate(((2, 1), (3, 0))):
                even = outer[2 * pair] * edge_sum + inner[2 * pair] * mid_sum
                uneven = outer[2 * pair + 1] * edge_diff + inner[2 * pair + 1] * mid_diff
                below = w_of(4 * (j - 1) + late, rows, even + uneven) if j > 0 else None
                above = w_of(4 * j + early, rows, even - uneven) if j < 8 else None
                if below is None:
                    sides.append((above, -above))
                elif above is None:
                    sides.append((below, below))
                else:
                    sides.append((below + above, below - above))
            (both0, differ0), (both1, differ1) = sides
            edge_even, edge_odd = outer[0] * both0 + outer[2] * both1, outer[1] * differ0 + outer[3] * differ1
            mid_even, mid_odd = inner[0] * both0 + inner[2] * both1, inner[1] * differ0 + inner[3] * differ1
            add(j, edge_even + edge_odd)
            add(j + 1, mid_even + mid_odd)
            add(j + 2, mid_even - mid_odd)
            add(j + 3, edge_even - edge_odd)
            for t in (j,) if j < 8 else (8, 9, 10, 11):
                down[pl.ds((t % 4) * cells + start, 8), (t // 4) * 128 : (t // 4 + 1) * 128] = back[t]
            x = [x[1], x[2], x[3], None]
        return carry

    if before_chunk is None:
        lax.fori_loop(0, cells // 8, tile, 0)
    else:
        for chunk in range(cells // CHUNK):
            before_chunk(chunk)
            lax.fori_loop(chunk * CHUNK // 8, (chunk + 1) * CHUNK // 8, tile, 0)
    high, low = split(down[...])
    both = dot(high, lon_down[...])
    narrow = both[:, :128] + both[:, 128:] + dot(low, lon_down[:, :128])
    narrow = jnp.concatenate([narrow[g * cells : (g + 1) * cells] for g in range(4)], axis=1)
    high, low = split(narrow)
    return dot(lat_down[...], jnp.concatenate([high, high, low], axis=0))


def finish(total, values, place):
    extra = penalty(values, place)
    sums = [group(total, g) + extra[g] for g in range(4)]
    turned = [jnp.concatenate([part, jnp.zeros((128 - ROWS, 128), jnp.float32)], axis=0).T for part in sums]
    return sums, [[turned[g][r * SEG : (r + 1) * SEG] for g in range(4)] for r in range(3)]


def write_ends(segs, place, tiles, first, second):
    lower = lax.broadcasted_iota(jnp.int32, (8, 128), 0) < 4
    for r in range(3):
        for g in range(4):
            tiles[r, g] = segs[r][g]
        for h in range(2):
            packed = [
                jnp.where(lower, segs[r][2 * h][at : at + 8], pltpu.roll(segs[r][2 * h + 1][at : at + 8], 4, 0))
                for at in (0, 32)
            ]
            first[r, h], second[r, h] = place.messages("lon", *packed)


def start_of(area, offset, precip, weight):
    def w_of(hour, rows, value):
        linear = offset[hour, rows, :] + value
        here = area[rows, :]
        w = here * jnp.exp((2.0 - tweedie_power) * linear)
        weight[hour, rows, :] = w
        return w - here * precip[hour, rows, :] * jnp.exp((1.0 - tweedie_power) * linear)

    return w_of


def start_middle_kernel(both, area, offset_far, precip_far, lat_up, lat_down, lon_up, lon_down,
                        weight, total, offset_edges, precip_edges, offset, precip, up, down, arrived):
    copies = []

    def bring(source, source_at, target, target_at, count):
        source, target = source.at[:, pl.ds(source_at, count), :], target.at[:, pl.ds(target_at, count), :]
        copies.append(pltpu.make_async_copy(source, target, arrived.at[len(copies)]))

    for chunk in range(CHUNKS):
        for source, target in ((offset_far, offset), (precip_far, precip)):
            bring(source, EDGE + chunk * CHUNK, target, chunk * CHUNK, CHUNK)
    for source, target in ((offset_far, offset_edges), (precip_far, precip_edges)):
        bring(source, 0, target, 0, EDGE)
        bring(source, LAT_CELLS - EDGE, target, EDGE, EDGE)
    for copy in copies:
        copy.start()

    def before_chunk(chunk):
        for copy in copies[2 * chunk : 2 * chunk + 2]:
            copy.wait()

    w_of = start_of(area, offset, precip, weight)
    total[...] = apply_cells(both[0], w_of, lat_up, lat_down, lon_up, lon_down, up, down, before_chunk)
    for copy in copies[2 * CHUNKS :]:
        copy.wait()


def start_kernel(both, got_first, got_second, total, area, offset, precip, lat_up, lat_down, lon_up, lon_down,
                 weight, diag, tiles, first, second, up, down):
    place = Place()
    row = lax.broadcasted_iota(jnp.int32, (8, LANES), 0)
    left, right = place.received("lat", got_first[...], got_second[...])

    def with_halo(own, left, right):
        head, tail = own[0:8] + jnp.where(row < 2, left, 0.0), own[64:72] + jnp.where((row >= 2) & (row < 4), right, 0.0)
        return jnp.concatenate([head, own[8:64], tail, own[72:80]], axis=0)

    values = with_halo(both[0], left, right)
    diag[...] = with_halo(both[1], pltpu.roll(left, 6, 0), pltpu.roll(right, 6, 0))
    w_of = start_of(area, offset, precip, weight)
    part = apply_cells(values, w_of, lat_up, lat_down, lon_up, lon_down, up, down)
    _, segs = finish(total[...] + part, values, place)
    write_ends(segs, place, tiles, first, second)


def weigh(weight):
    return lambda hour, rows, value: weight[hour, rows, :] * value


def hessian_middle_kernel(partial_rows, diag, weight, lat_up, lat_down, lon_up, lon_down, total, up, down, *, again):
    here = partial_rows[...] if again else -partial_rows[...]
    total[...] = apply_cells(diag[...] * here, weigh(weight), lat_up, lat_down, lon_up, lon_down, up, down)


def hessian_kernel(partial_rows, got_first, got_second, total, diag, weight, lat_up, lat_down, lon_up, lon_down, *refs, again):
    if again:
        before, residual, scaled, tiles, slots, up, down = refs
    else:
        residual, scaled, tiles, first, second, sums, up, down = refs
    place = Place()
    merged = merge_rows(partial_rows[...], got_first[...], got_second[...], place)
    here = merged if again else -merged
    residual[...] = here
    values = diag[...] * here
    scaled[...] = values
    part = apply_cells(values, weigh(weight), lat_up, lat_down, lon_up, lon_down, up, down)
    image, segs = finish(total[...] + part, values, place)
    lines = [own_lane_sum(here * values), lane_sum([image[g] * group(values, g) for g in range(4)])]
    if again:
        for r in range(3):
            for g in range(4):
                tiles[r, g] = segs[r][g]
        lines = jnp.concatenate([jnp.zeros((4, 128), jnp.float32), before[0:2], *lines], axis=0)
        write_slots(image, segs, lines, slots)
    else:
        write_ends(segs, place, tiles, first, second)
        sums[...] = jnp.concatenate(lines + [jnp.zeros((6, 128), jnp.float32)], axis=0)


def slot_at(lon_step, lat_step):
    lon_count, lat_count = lax.axis_size("lon"), lax.axis_size("lat")
    lon = lax.rem(lax.axis_index("lon") + (lon_count + lon_step), lon_count)
    return lon * lat_count + lax.rem(lax.axis_index("lat") + (lat_count + lat_step), lat_count)


def rolled(values, amount, axis):
    amount %= values.shape[axis]
    return pltpu.roll(values, amount, axis) if amount else values


def row_of(shape=(8, 128)):
    return lax.broadcasted_iota(jnp.int32, shape, 0)


def write_slots(sums, segs, lines, slots):
    row = row_of()
    low = lax.broadcasted_iota(jnp.int32, (8, 128), 1) < LAT_OWN
    for j in range(slots.shape[0]):
        slots[j, 0:8] = jnp.zeros((8, 128), jnp.float32)
        slots[j, 8:16] = lines
    for step, at, skip in ((-1, 0, 0), (1, 32, 2)):
        halves_of = [jnp.zeros((8, 128), jnp.float32), lines]
        for r in range(3):
            for h in range(2):
                index = 2 * r + h
                pair = jnp.where(
                    low, pltpu.roll(segs[r][2 * h][at : at + 8], 126, 1), pltpu.roll(segs[r][2 * h + 1][at : at + 8], 62, 1)
                )
                to = 2 * (index % 4)
                part = rolled(pair, to - skip, 0)
                halves_of[index // 4] = jnp.where((row >= to) & (row < to + 2), part, halves_of[index // 4])
        slot = slot_at(step, 0)
        slots[slot, 0:8] = halves_of[0]
        slots[slot, 8:16] = halves_of[1]
    for lat_step, at, skip in ((-1, 0, 0), (1, 64, 2)):
        content = jnp.zeros((8, 128), jnp.float32)
        for g in range(4):
            part = rolled(sums[g][at : at + 8], 2 * g - skip, 0)
            content = jnp.where((row >= 2 * g) & (row < 2 * g + 2), part, content)
        for lon_step in (-1, 0, 1):
            slots[slot_at(lon_step, lat_step), 0:8] = content


def collect_kernel(tiles, slots, merged, first, second, lines):
    place = Place()
    row = row_of()
    lane = lax.broadcasted_iota(jnp.int32, (8, 128), 1)
    own_lane = within(lane, LAT_OWN)
    r_of = (lane >= SEG).astype(jnp.int32) + (lane >= 2 * SEG).astype(jnp.int32)
    lon = lane - SEG * r_of
    sides = []
    for lat_step, share in ((-1, place.left["lat"]), (1, place.right["lat"])):
        before, same, after = (slots[slot_at(lon_step, lat_step), 0:8] for lon_step in (-1, 0, 1))
        side = jnp.where(within(lon, LON_OWN), same, 0.0)
        side = side + jnp.where(within(lon, 2), pltpu.roll(before, 128 - LON_OWN, 1), 0.0)
        side = side + jnp.where((lon >= LON_OWN) & (lon < LON_OWN + 2), pltpu.roll(after, LON_OWN, 1), 0.0)
        sides.append(side * share)
    blank = jnp.zeros((56, 128), jnp.float32)
    from_lat = []
    for g in range(4):
        head = jnp.where(within(row, 2), rolled(sides[0], 2 - 2 * g, 0), 0.0)
        tail = jnp.where(row < 2, rolled(sides[1], -2 * g, 0), 0.0)
        from_lat.append(jnp.concatenate([head, blank, tail, blank], axis=0).T)
    left = [slots[slot_at(-1, 0), at : at + 8] for at in (0, 8)]
    right = [slots[slot_at(1, 0), at : at + 8] for at in (0, 8)]
    for r in range(3):
        for g in range(4):
            index = 2 * r + g // 2
            shift = 66 if g % 2 else 2
            to = 2 * (index % 4)
            head = jnp.where(within(row, 2) & own_lane, pltpu.roll(rolled(left[index // 4], 2 - to, 0), shift, 1), 0.0)
            tail = jnp.where((row < 2) & own_lane, pltpu.roll(rolled(right[index // 4], -to, 0), shift, 1), 0.0)
            seg = tiles[r, g] + from_lat[g][r * SEG : (r + 1) * SEG]
            merged[r, g] = jnp.concatenate([seg[0:8] + head, seg[8:32], seg[32:40] + tail], axis=0)
    total = slots[0, 8:16]
    for j in range(1, slots.shape[0]):
        total = total + slots[j, 8:16]
    lines[...] = total
    low = lax.broadcasted_iota(jnp.int32, (SEG, 128), 1) < LAT_OWN

    def message(r, g):
        data = jnp.where(low, pltpu.roll(merged[r, g], 126, 1), pltpu.roll(merged[r, g + 1], 62, 1))
        return jnp.concatenate([data[:32], jnp.where(row < 4, data[32:], total)], axis=0)

    first[...], second[...] = place.messages("tm", message(0, 0), message(2, 2))


def join_kernel(tiles, got_first, got_second, joined, first, second):
    place = Place()
    lower = lax.broadcasted_iota(jnp.int32, (8, 128), 0) < 4
    for r in range(3):
        for g in range(4):
            left, right = place.received("lon", got_first[r, g // 2], got_second[r, g // 2])
            if g % 2:
                left, right = pltpu.roll(left, 4, 0), pltpu.roll(right, 4, 0)
            joined[r, g, 0:8] = tiles[r, g, 0:8] + jnp.where(lower, left, 0.0)
            joined[r, g, 8:32] = tiles[r, g, 8:32]
            joined[r, g, 32:40] = tiles[r, g, 32:40] + jnp.where(lower, right, 0.0)
    for g in range(4):
        first[g], second[g] = place.messages("tm", joined[0, g], joined[2, g])


def turned_rows(tiles, g, left=0.0, right=0.0):
    parts = [tiles[0, g] + left, tiles[1, g], tiles[2, g] + right, jnp.zeros((8, 128), jnp.float32)]
    return jnp.concatenate(parts, axis=0).T


def turn_kernel(tiles, got_first, got_second, rows, first, second):
    place = Place()
    for g in range(4):
        block = turned_rows(tiles, g, *place.received("tm", got_first[g], got_second[g]))
        lanes = slice(g * 128, (g + 1) * 128)
        rows[:, lanes] = block[:ROWS]
        first[:, lanes], second[:, lanes] = place.messages("lat", block[0:8], block[64:72])


def embed_kernel(coefficients, inverse_diag, tiles, first, second):
    place = Place()
    pair = lax.broadcasted_iota(jnp.int32, (8, 128), 0) // 2
    heads, tails = [None] * 4, [None] * 4
    for t in range(12):
        for k, values in enumerate((coefficients, inverse_diag)):
            if 2 <= t < T_OWN + 2:
                own = jnp.concatenate([values[t - 2], jnp.zeros((LON_OWN, 128 - LAT_OWN), jnp.float32)], axis=1)
                own = jnp.concatenate([own, jnp.zeros((SEG - LON_OWN, 128), jnp.float32)], axis=0)
                seg = pltpu.roll(pltpu.roll(own, 2, 0), 2, 1)
                at, tile = 2 * (t % 2) + k, (t - 2) // 2
                head, tail = rolled(seg[0:8], 2 * at - 2, 0), rolled(seg[32:40], 2 * at, 0)
                heads[tile] = head if at == 0 else jnp.where(pair == at, head, heads[tile])
                tails[tile] = tail if at == 0 else jnp.where(pair == at, tail, tails[tile])
            else:
                seg = jnp.zeros((SEG, 128), jnp.float32)
            tiles[k, t // 4, t % 4] = seg
    for tile in range(4):
        first[tile], second[tile] = place.messages("lon", heads[tile], tails[tile])


def embed_join_kernel(tiles, got_first, got_second, joined, first, second):
    place = Place()
    row = lax.broadcasted_iota(jnp.int32, (8, 128), 0)
    for k in range(2):
        for t in range(12):
            r, g = t // 4, t % 4
            if 2 <= t < T_OWN + 2:
                at, tile = 2 * (t % 2) + k, (t - 2) // 2
                left, right = place.received("lon", got_first[tile], got_second[tile])
                left, right = rolled(left, -2 * at, 0), rolled(right, 2 - 2 * at, 0)
                joined[k, r, g, 0:8] = tiles[k, r, g, 0:8] + jnp.where(row < 2, left, 0.0)
                joined[k, r, g, 8:32] = tiles[k, r, g, 8:32]
                joined[k, r, g, 32:40] = tiles[k, r, g, 32:40] + jnp.where((row >= 2) & (row < 4), right, 0.0)
            else:
                joined[k, r, g] = tiles[k, r, g]
    low = lax.broadcasted_iota(jnp.int32, (SEG, 128), 1) < LAT_OWN

    def beside(r, g):
        return jnp.where(low, pltpu.roll(joined[0, r, g], 126, 1), pltpu.roll(joined[1, r, g], 62, 1))

    for i in range(2):
        first[i], second[i] = place.messages("tm", beside(0, 2 + i), beside(2, i))


def embed_turn_kernel(tiles, got_first, got_second, rows, first, second):
    place = Place()
    lane = lax.broadcasted_iota(jnp.int32, (SEG, 128), 1)
    own = (lane >= 2) & (lane < LAT_OWN + 2)
    row = lax.broadcasted_iota(jnp.int32, (8, 128), 0)
    for g in range(4):
        lanes = slice(g * 128, (g + 1) * 128)
        left, right = place.received("tm", got_first[g % 2], got_second[g % 2])
        blocks = []
        for k in range(2):
            shift = 66 if k else 2
            if g < 2:
                block = turned_rows(tiles.at[k], g, left=jnp.where(own, pltpu.roll(left, shift, 1), 0.0))
            else:
                block = turned_rows(tiles.at[k], g, right=jnp.where(own, pltpu.roll(right, shift, 1), 0.0))
            rows[k, :, lanes] = block[:ROWS]
            blocks.append(block)
        head = jnp.where(row < 4, blocks[0][0:8], pltpu.roll(blocks[1][0:8], 2, 0))
        tail = jnp.where(row < 2, blocks[0][64:72], pltpu.roll(blocks[1][64:72], 2, 0))
        first[:, lanes], second[:, lanes] = place.messages("lat", head, tail)


def last_kernel(tiles, got_first, got_second, lines, got_lines, residual, scaled, image, image_scaled, step_out, residual_out):
    place = Place()
    left, right = place.received("tm", got_first[...], got_second[...])
    lane = lax.broadcasted_iota(jnp.int32, (SEG, 128), 1)
    own = within(lane, LAT_OWN)
    merged = []
    for g in range(4):
        side = right if g < 2 else left
        side = jnp.where(own, pltpu.roll(side, 66 if g % 2 else 2, 1), 0.0)
        block = turned_rows(tiles, g, right=side) if g < 2 else turned_rows(tiles, g, left=side)
        merged.append(block[:ROWS])
    merged = jnp.concatenate(merged, axis=1)
    total = lines[...] + got_lines[...] + got_first[32:40] + got_second[32:40]
    norm, curvature, image_norm, image_curvature = (jnp.sum(total[i : i + 1], axis=1, keepdims=True) for i in range(4, 8))
    step_size = norm / curvature
    next_norm = step_size * step_size * image_norm - norm
    ratio = next_norm / norm
    next_curvature = curvature - 2.0 * step_size * image_norm + step_size * step_size * image_curvature
    step_next = next_norm / (next_curvature - ratio * next_norm / step_size)
    direction = scaled[...] - step_size * image_scaled[...] + ratio * scaled[...]
    newton = step_size * scaled[...] + step_next * direction
    left_over = residual[...] - step_size * image[...] - step_next * (image[...] - step_size * merged + ratio * image[...])
    for values, out in ((newton, step_out), (left_over, residual_out)):
        for g in range(4):
            turned = jnp.concatenate([group(values, g), jnp.zeros((128 - ROWS, 128), jnp.float32)], axis=0).T
            turned = pltpu.roll(turned, 126, 1)
            for r in range(3):
                t = 4 * r + g - 2
                if 0 <= t < T_OWN:
                    out[t] = pltpu.roll(turned[r * SEG : (r + 1) * SEG], SEG - 2, 0)[:LON_OWN, :LAT_OWN]


def matchings(count):
    return [(i, (((i + 1) ^ 1) - 1) % count) for i in range(count)], [(i, i ^ 1) for i in range(count)]


def swap(first, second, axis):
    first_pairs, second_pairs = matchings(lax.axis_size(axis))
    return lax.ppermute(first, axis, first_pairs), lax.ppermute(second, axis, second_pairs)


def shaped(*shape):
    return jax.ShapeDtypeStruct(shape, jnp.float32)


def call(kernel, out_shape, name, *args, scratch=(), far=(), limit=24):
    vmem = pl.BlockSpec(memory_space=pltpu.VMEM)
    hbm = pl.BlockSpec(memory_space=pltpu.HBM)
    return pl.pallas_call(
        kernel,
        in_specs=[hbm if i in far else vmem for i in range(len(args))],
        out_specs=[vmem] * len(out_shape),
        out_shape=out_shape,
        scratch_shapes=scratch,
        compiler_params=pltpu.CompilerParams(vmem_limit_bytes=limit * 1024 * 1024),
        cost_estimate=pl.CostEstimate(flops=10**9, bytes_accessed=20 * 10**6, transcendentals=0),
        name=name,
    )(*args)


LON_MESSAGE, TM_MESSAGE, LAT_MESSAGE = (3, 2, 8, 128), (4, SEG, 128), (8, LANES)
TILES = (3, 4, SEG, 128)
VECTOR = (ROWS, LANES)
MID_SCRATCH, EDGE_SCRATCH = ([pltpu.VMEM((4 * n, 384), jnp.float32)] * 2 for n in (MID_CELLS, EDGE_CELLS))
MID, ENDS = ((HOURS, n, LON_CELLS) for n in (MID_CELLS, EDGE_CELLS))


def exchange(tiles, first, second):
    first, second = swap(first, second, "lon")
    tiles, first, second = call(
        join_kernel, (shaped(*TILES), shaped(*TM_MESSAGE), shaped(*TM_MESSAGE)), "join", tiles, first, second
    )
    first, second = swap(first, second, "tm")
    rows, first, second = call(
        turn_kernel, (shaped(*VECTOR), shaped(*LAT_MESSAGE), shaped(*LAT_MESSAGE)), "turn", tiles, first, second
    )
    return rows, *swap(first, second, "lat")


def fold_and_sum(tiles, slots, lines_shape):
    slots = lax.all_to_all(slots, ("lon", "lat"), 0, 0, tiled=True)
    message = shaped(SEG, 128)
    tiles, first, second, lines = call(
        collect_kernel, (shaped(*TILES), message, message, lines_shape), "collect", tiles, slots
    )
    first, second = swap(first, second, "tm")
    count = lax.axis_size("tm")
    return tiles, first, second, lines, lax.ppermute(lines, "tm", [(i, (i + 2) % count) for i in range(count)])


def expand(coefficients, inverse_diag):
    tiles, message = shaped(2, *TILES), shaped(4, 8, 128)
    tiles_here, first, second = call(
        embed_kernel, (tiles, message, message), "embed", coefficients, inverse_diag
    )
    first, second = swap(first, second, "lon")
    message = shaped(2, SEG, 128)
    tiles_here, first, second = call(embed_join_kernel, (tiles, message, message), "embed_join", tiles_here, first, second)
    first, second = swap(first, second, "tm")
    shapes = (shaped(2, *VECTOR), shaped(*LAT_MESSAGE), shaped(*LAT_MESSAGE))
    both, first, second = call(embed_turn_kernel, shapes, "embed_turn", tiles_here, first, second)
    return both, *swap(first, second, "lat")


def per_device(precip, offset, coefficients, inverse_diag):
    lat_total = LAT_CELLS * lax.axis_size("lat")
    lat_index = (lax.axis_index("lat") * LAT_CELLS + jnp.arange(LAT_CELLS, dtype=jnp.int32)).astype(jnp.float32)
    area = jnp.cos((90.0 - (lat_index + 0.5) * 180.0 / lat_total) * (jnp.pi / 180.0))
    area = jnp.broadcast_to(area[:, None], (LAT_CELLS, LON_CELLS))
    mid_tabs, edge_tabs = tables()
    ends = (shaped(*TILES), shaped(*LON_MESSAGE), shaped(*LON_MESSAGE))
    vector = shaped(*VECTOR)

    both, *got = expand(coefficients.transpose(0, 2, 1), inverse_diag.transpose(0, 2, 1))
    weight, total, offset_edges, precip_edges = call(
        start_middle_kernel, (shaped(*MID), vector, shaped(*ENDS), shaped(*ENDS)), "start_middle",
        both, middle(area), offset, precip, *mid_tabs,
        scratch=[pltpu.VMEM(MID, jnp.float32)] * 2 + MID_SCRATCH + [pltpu.SemaphoreType.DMA((2 * CHUNKS + 4,))],
        far=(2, 3), limit=47,
    )
    edge_weight, diag, *sent = call(
        start_kernel, (shaped(*ENDS), vector, *ends), "start", both, *got, total, edges(area), offset_edges, precip_edges,
        *edge_tabs, scratch=EDGE_SCRATCH,
    )

    def hessian(again, rows, got, outs, *more):
        total, = call(
            functools.partial(hessian_middle_kernel, again=again), (vector,), "hessian_middle", rows, diag, weight, *mid_tabs,
            scratch=MID_SCRATCH,
        )
        return call(
            functools.partial(hessian_kernel, again=again), (vector, vector, *outs), "hessian", rows, *got, total, diag,
            edge_weight, *edge_tabs, *more, scratch=EDGE_SCRATCH,
        )

    lines = shaped(8, 128)
    rows, *got = exchange(*sent)
    residual, scaled, *sent, sums = hessian(False, rows, got, (*ends, lines))
    slots = shaped(lax.axis_size("lon") * lax.axis_size("lat"), 16, 128)
    rows, *got = exchange(*sent)
    image, image_scaled, tiles, slots = hessian(True, rows, got, (ends[0], slots), sums)
    out = shaped(T_OWN, LON_OWN, LAT_OWN)
    outs = call(
        last_kernel, (out, out), "last", *fold_and_sum(tiles, slots, lines), residual, scaled, image, image_scaled
    )
    return tuple(v.transpose(0, 2, 1) for v in outs)


def solution(mesh):
    return jax.shard_map(
        per_device, mesh=mesh, in_specs=(P(*SPLIT),) * 4, out_specs=(P(*SPLIT),) * 2, check_vma=False
    )
```

```python
import functools

import jax
import jax.numpy as jnp
import numpy as np
from jax import lax
from jax.experimental import pallas as pl
from jax.experimental.pallas import tpu as pltpu
from jax.sharding import PartitionSpec as P

SPLIT = ("tm", "lat", "lon")
tweedie_power = 1.6
smooth = 0.5

ROWS, LANES, SEG, LAT_OWN, LON_OWN, T_OWN = 80, 512, 40, 64, 32, 8
HOURS, LAT_CELLS, LON_CELLS = 32, 256, 128
EDGE, CHUNK = 16, 112
MID_CELLS, EDGE_CELLS = LAT_CELLS - 2 * EDGE, 2 * EDGE


def spline(offsets):
    distance = np.abs(offsets)
    near_part = (4.0 - 6.0 * distance**2 + 3.0 * distance**3) / 6.0
    far_part = np.maximum(2.0 - distance, 0.0) ** 3 / 6.0
    return np.where(distance < 1.0, near_part, far_part)


def table(cell_count, knot_count):
    cell_pos = np.arange(cell_count, dtype=np.float64)[:, None]
    knot_pos = np.arange(knot_count + 4, dtype=np.float64)[None, :] - 2.0
    return spline((cell_pos - 4.0 * knot_pos - 1.5) / 4.0)


def halves(values):
    values = jnp.asarray(values, jnp.float32)
    high = values.astype(jnp.bfloat16)
    return high, (values - high.astype(jnp.float32)).astype(jnp.bfloat16)


def middle(cells, axis=0):
    return lax.slice_in_dim(cells, EDGE, LAT_CELLS - EDGE, axis=axis)


def edges(cells, axis=0):
    ends = (lax.slice_in_dim(cells, at, at + EDGE, axis=axis) for at in (0, LAT_CELLS - EDGE))
    return jnp.concatenate(list(ends), axis=axis)


def tables():
    lat = np.zeros((LAT_CELLS, ROWS))
    lat[:, : LAT_OWN + 4] = table(LAT_CELLS, LAT_OWN)
    high, low = halves(lat)
    lat_tables = []
    for part in (middle, edges):
        up = jnp.concatenate([part(high), part(low), part(high)], axis=1)
        cells = CHUNK if part is middle else EDGE_CELLS
        down = [p.reshape(-1, cells, ROWS).transpose(0, 2, 1) for p in (part(high), part(low))]
        lat_tables += [up, jnp.concatenate([down[0], down[1], down[0]], axis=2)]
    lon = np.zeros((128, 3 * LON_CELLS))
    for r in range(3):
        lon[r * SEG : r * SEG + LON_OWN + 4, r * LON_CELLS : (r + 1) * LON_CELLS] = table(LON_CELLS, LON_OWN).T
    high, low = halves(lon)
    lon_up = jnp.concatenate([high, high, low], axis=0)
    lon_down = jnp.concatenate([high.T, low.T], axis=1)
    return lat_tables[:2] + [lon_up, lon_down], lat_tables[2:] + [lon_up, lon_down]


def hour_factors():
    near, far = ([float(spline(np.float64(x))) for x in xs] for xs in ((0.125, 0.875, 0.375, 0.625), (1.125, 1.875, 1.375, 1.625)))
    outer = ((far[0] + far[1]) / 2, (far[0] - far[1]) / 2, (far[2] + far[3]) / 2, (far[2] - far[3]) / 2)
    inner = ((near[0] + near[1]) / 2, (near[0] - near[1]) / 2, (near[2] + near[3]) / 2, (near[2] - near[3]) / 2)
    return outer, inner


class Place:
    def __init__(self):
        index = {axis: lax.axis_index(axis) for axis in SPLIT}
        self.even = {axis: index[axis] % 2 == 0 for axis in SPLIT}
        self.left = {axis: jnp.where(index[axis] > 0, 1.0, 0.0) for axis in SPLIT}
        self.right = {axis: jnp.where(index[axis] < lax.axis_size(axis) - 1, 1.0, 0.0) for axis in SPLIT}

    def messages(self, axis, to_left, to_right):
        return jnp.where(self.even[axis], to_left, to_right), jnp.where(self.even[axis], to_right, to_left)

    def received(self, axis, first, second):
        left, right = jnp.where(self.even[axis], first, second), jnp.where(self.even[axis], second, first)
        return (left, right) if axis == "lon" else (left * self.left[axis], right * self.right[axis])


def split(values):
    high = values.astype(jnp.bfloat16)
    return high, (values - high.astype(jnp.float32)).astype(jnp.bfloat16)


def dot(left, right):
    return jnp.dot(left, right, preferred_element_type=jnp.float32)


def lane_places():
    lane = lax.broadcasted_iota(jnp.int32, (ROWS, 128), 1)
    r = (lane >= SEG).astype(jnp.int32) + (lane >= 2 * SEG).astype(jnp.int32)
    return r, lane - SEG * r, lax.broadcasted_iota(jnp.int32, (ROWS, 128), 0)


def within(place, count):
    return (place >= 2) & (place < count + 2)


def group(values, g):
    return values[:, g * 128 : (g + 1) * 128]


def penalty(values, place):
    r, lon, row = lane_places()
    own_row, own_lon = within(row, LAT_OWN), within(lon, LON_OWN)
    row_share = jnp.where(
        own_row, 1.0, jnp.where(row == 1, 1.0 - place.left["lat"], jnp.where(row == LAT_OWN + 2, 1.0 - place.right["lat"], 0.0))
    )
    parts = [group(values, g) for g in range(4)]

    def along_t(v):
        before = [pltpu.roll(v[3], SEG, 1), v[0], v[1], v[2]]
        after = [v[1], v[2], v[3], pltpu.roll(v[0], 128 - SEG, 1)]
        return [b - 2.0 * m + a for b, m, a in zip(before, v, after)]

    t_second = along_t(parts)
    t_shared = []
    summed = []
    for g in range(4):
        t = 4 * r + g
        own_t = within(t, T_OWN)
        share = jnp.where(own_t, 1.0, jnp.where(t == 1, 1.0 - place.left["tm"], jnp.where(t == T_OWN + 2, 1.0 - place.right["tm"], 0.0)))
        t_shared.append(jnp.where(own_row & own_lon, share, 0.0) * t_second[g])
        v = parts[g]
        second = pltpu.roll(v, 1, 0) - 2.0 * v + pltpu.roll(v, ROWS - 1, 0)
        second = jnp.where(own_t & own_lon, row_share, 0.0) * second
        total = pltpu.roll(second, 1, 0) - 2.0 * second + pltpu.roll(second, ROWS - 1, 0)
        second = pltpu.roll(v, 1, 1) - 2.0 * v + pltpu.roll(v, 127, 1)
        second = jnp.where(own_t & own_lon & own_row, second, 0.0)
        summed.append(total + pltpu.roll(second, 1, 1) - 2.0 * second + pltpu.roll(second, 127, 1))
    return [smooth * (a + b) for a, b in zip(summed, along_t(t_shared))]


def lane_sum(parts):
    return jnp.sum(parts[0] + parts[1] + parts[2] + parts[3], axis=0, keepdims=True)


def own_lane_sum(values):
    r, lon, row = lane_places()
    inside = within(row, LAT_OWN) & within(lon, LON_OWN)
    return lane_sum([jnp.where(inside & within(4 * r + g, T_OWN), group(values, g), 0.0) for g in range(4)])


def merge_rows(values, got_first, got_second, place):
    keep = lax.broadcasted_iota(jnp.int32, (8, LANES), 0) < 4
    left, right = place.received("lat", got_first, got_second)
    return jnp.concatenate(
        [
            values[0:8] + jnp.where(keep, left, 0.0),
            values[8:64],
            values[64:72] + jnp.where(keep, right, 0.0),
            values[72:80],
        ],
        axis=0,
    )


def expand_cells(parts, lat_up, lon_up, up):
    expanded = dot(lat_up, parts)
    high, low = split(jnp.concatenate([group(expanded, g) for g in range(4)], axis=0))
    up[...] = dot(jnp.concatenate([high, low, high], axis=1), lon_up[...])


def cells_tile(w_of, first_row, start, cells, up, down):
    outer, inner = hour_factors()
    rows = pl.ds(first_row + start, 8)

    def knot(t):
        return up[pl.ds((t % 4) * cells + start, 8), (t // 4) * 128 : (t // 4 + 1) * 128]

    back = [None] * 12

    def add(t, value):
        back[t] = value if back[t] is None else back[t] + value

    x = [knot(0), knot(1), knot(2), None]
    for j in range(9):
        x[3] = knot(j + 3)
        edge_sum, edge_diff, mid_sum, mid_diff = x[0] + x[3], x[0] - x[3], x[1] + x[2], x[1] - x[2]
        sides = []
        for pair, (late, early) in enumerate(((2, 1), (3, 0))):
            even = outer[2 * pair] * edge_sum + inner[2 * pair] * mid_sum
            uneven = outer[2 * pair + 1] * edge_diff + inner[2 * pair + 1] * mid_diff
            below = w_of(4 * (j - 1) + late, rows, even + uneven) if j > 0 else None
            above = w_of(4 * j + early, rows, even - uneven) if j < 8 else None
            if below is None:
                sides.append((above, -above))
            elif above is None:
                sides.append((below, below))
            else:
                sides.append((below + above, below - above))
        (both0, differ0), (both1, differ1) = sides
        edge_even, edge_odd = outer[0] * both0 + outer[2] * both1, outer[1] * differ0 + outer[3] * differ1
        mid_even, mid_odd = inner[0] * both0 + inner[2] * both1, inner[1] * differ0 + inner[3] * differ1
        add(j, edge_even + edge_odd)
        add(j + 1, mid_even + mid_odd)
        add(j + 2, mid_even - mid_odd)
        add(j + 3, edge_even - edge_odd)
        for t in (j,) if j < 8 else (8, 9, 10, 11):
            down[pl.ds((t % 4) * cells + start, 8), (t // 4) * 128 : (t // 4 + 1) * 128] = back[t]
        x = [x[1], x[2], x[3], None]


def fold_cells(down, cells, lat_down, lon_down):
    high, low = split(down[...])
    both = dot(high, lon_down[...])
    narrow = both[:, :128] + both[:, 128:] + dot(low, lon_down[:, :128])
    narrow = jnp.concatenate([narrow[g * cells : (g + 1) * cells] for g in range(4)], axis=1)
    high, low = split(narrow)
    return dot(lat_down, jnp.concatenate([high, high, low], axis=0))


def apply_cells(values, w_of, lat_up, lat_down, lon_up, lon_down, *scratch):
    high, low = split(values)
    parts = jnp.concatenate([high, high, low], axis=0)
    chunks, _, _ = lat_down.shape
    cells = lat_up.shape[0] // chunks
    buffers = scratch[:2], scratch[2:]
    expand_cells(parts, lat_up[0:cells], lon_up, buffers[0][0])
    total = None
    for chunk in range(chunks):
        up, down = buffers[chunk % 2]
        if chunk + 1 < chunks:
            expand_cells(parts, lat_up[(chunk + 1) * cells : (chunk + 2) * cells], lon_up, buffers[(chunk + 1) % 2][0])
        for start in range(0, cells, 8):
            cells_tile(w_of, chunk * cells, start, cells, up, down)
        part = fold_cells(down, cells, lat_down[chunk], lon_down)
        total = part if total is None else total + part
    return total


def finish(total, values, place):
    extra = penalty(values, place)
    sums = [group(total, g) + extra[g] for g in range(4)]
    turned = [jnp.concatenate([part, jnp.zeros((128 - ROWS, 128), jnp.float32)], axis=0).T for part in sums]
    return sums, [[turned[g][r * SEG : (r + 1) * SEG] for g in range(4)] for r in range(3)]


def write_ends(segs, place, tiles, first, second):
    lower = lax.broadcasted_iota(jnp.int32, (8, 128), 0) < 4
    for r in range(3):
        for g in range(4):
            tiles[r, g] = segs[r][g]
        for h in range(2):
            packed = [
                jnp.where(lower, segs[r][2 * h][at : at + 8], pltpu.roll(segs[r][2 * h + 1][at : at + 8], 4, 0))
                for at in (0, 32)
            ]
            first[r, h], second[r, h] = place.messages("lon", *packed)


def start_of(area, offset, precip, weight):
    def w_of(hour, rows, value):
        linear = offset[hour, rows, :] + value
        here = area[rows, :]
        w = here * jnp.exp((2.0 - tweedie_power) * linear)
        weight[hour, rows, :] = w
        return w - here * precip[hour, rows, :] * jnp.exp((1.0 - tweedie_power) * linear)

    return w_of


def load_kernel(_, offset_far, precip_far, offset, precip, offset_edges, precip_edges, arrived):
    copies = []

    def bring(source, source_at, target, target_at, count):
        source, target = source.at[:, pl.ds(source_at, count), :], target.at[:, pl.ds(target_at, count), :]
        copies.append(pltpu.make_async_copy(source, target, arrived.at[len(copies)]))

    for source, target, ends in ((offset_far, offset, offset_edges), (precip_far, precip, precip_edges)):
        bring(source, EDGE, target, 0, MID_CELLS)
        bring(source, 0, ends, 0, EDGE)
        bring(source, LAT_CELLS - EDGE, ends, EDGE, EDGE)
    for copy in copies:
        copy.start()
    for copy in copies:
        copy.wait()


def start_middle_kernel(both, area, offset, precip, lat_up, lat_down, lon_up, lon_down, weight, total, *scratch):
    w_of = start_of(area, offset, precip, weight)
    total[...] = apply_cells(both[0], w_of, lat_up, lat_down, lon_up, lon_down, *scratch)


def start_kernel(both, got_first, got_second, total, area, offset, precip, lat_up, lat_down, lon_up, lon_down,
                 weight, diag, tiles, first, second, *scratch):
    place = Place()
    row = lax.broadcasted_iota(jnp.int32, (8, LANES), 0)
    left, right = place.received("lat", got_first[...], got_second[...])

    def with_halo(own, left, right):
        head, tail = own[0:8] + jnp.where(row < 2, left, 0.0), own[64:72] + jnp.where((row >= 2) & (row < 4), right, 0.0)
        return jnp.concatenate([head, own[8:64], tail, own[72:80]], axis=0)

    values = with_halo(both[0], left, right)
    diag[...] = with_halo(both[1], pltpu.roll(left, 6, 0), pltpu.roll(right, 6, 0))
    w_of = start_of(area, offset, precip, weight)
    part = apply_cells(values, w_of, lat_up, lat_down, lon_up, lon_down, *scratch)
    _, segs = finish(total[...] + part, values, place)
    write_ends(segs, place, tiles, first, second)


def weigh(weight):
    return lambda hour, rows, value: weight[hour, rows, :] * value


def hessian_middle_kernel(partial_rows, diag, weight, lat_up, lat_down, lon_up, lon_down, total, *scratch, again):
    here = partial_rows[...] if again else -partial_rows[...]
    total[...] = apply_cells(diag[...] * here, weigh(weight), lat_up, lat_down, lon_up, lon_down, *scratch)


def hessian_kernel(partial_rows, got_first, got_second, total, diag, weight, lat_up, lat_down, lon_up, lon_down, *refs, again):
    if again:
        before, residual, scaled, tiles, slots, *scratch = refs
    else:
        residual, scaled, tiles, first, second, sums, *scratch = refs
    place = Place()
    merged = merge_rows(partial_rows[...], got_first[...], got_second[...], place)
    here = merged if again else -merged
    residual[...] = here
    values = diag[...] * here
    scaled[...] = values
    part = apply_cells(values, weigh(weight), lat_up, lat_down, lon_up, lon_down, *scratch)
    image, segs = finish(total[...] + part, values, place)
    lines = [own_lane_sum(here * values), lane_sum([image[g] * group(values, g) for g in range(4)])]
    if again:
        for r in range(3):
            for g in range(4):
                tiles[r, g] = segs[r][g]
        lines = jnp.concatenate([jnp.zeros((4, 128), jnp.float32), before[0:2], *lines], axis=0)
        write_slots(image, segs, lines, slots)
    else:
        write_ends(segs, place, tiles, first, second)
        sums[...] = jnp.concatenate(lines + [jnp.zeros((6, 128), jnp.float32)], axis=0)


def slot_at(lon_step, lat_step):
    lon_count, lat_count = lax.axis_size("lon"), lax.axis_size("lat")
    lon = lax.rem(lax.axis_index("lon") + (lon_count + lon_step), lon_count)
    return lon * lat_count + lax.rem(lax.axis_index("lat") + (lat_count + lat_step), lat_count)


def rolled(values, amount, axis):
    amount %= values.shape[axis]
    return pltpu.roll(values, amount, axis) if amount else values


def row_of(shape=(8, 128)):
    return lax.broadcasted_iota(jnp.int32, shape, 0)


def write_slots(sums, segs, lines, slots):
    row = row_of()
    low = lax.broadcasted_iota(jnp.int32, (8, 128), 1) < LAT_OWN
    for j in range(slots.shape[0]):
        slots[j, 0:8] = jnp.zeros((8, 128), jnp.float32)
        slots[j, 8:16] = lines
    for step, at, skip in ((-1, 0, 0), (1, 32, 2)):
        halves_of = [jnp.zeros((8, 128), jnp.float32), lines]
        for r in range(3):
            for h in range(2):
                index = 2 * r + h
                pair = jnp.where(
                    low, pltpu.roll(segs[r][2 * h][at : at + 8], 126, 1), pltpu.roll(segs[r][2 * h + 1][at : at + 8], 62, 1)
                )
                to = 2 * (index % 4)
                part = rolled(pair, to - skip, 0)
                halves_of[index // 4] = jnp.where((row >= to) & (row < to + 2), part, halves_of[index // 4])
        slot = slot_at(step, 0)
        slots[slot, 0:8] = halves_of[0]
        slots[slot, 8:16] = halves_of[1]
    for lat_step, at, skip in ((-1, 0, 0), (1, 64, 2)):
        content = jnp.zeros((8, 128), jnp.float32)
        for g in range(4):
            part = rolled(sums[g][at : at + 8], 2 * g - skip, 0)
            content = jnp.where((row >= 2 * g) & (row < 2 * g + 2), part, content)
        for lon_step in (-1, 0, 1):
            slots[slot_at(lon_step, lat_step), 0:8] = content


def collect_kernel(tiles, slots, merged, first, second, lines):
    place = Place()
    row = row_of()
    lane = lax.broadcasted_iota(jnp.int32, (8, 128), 1)
    own_lane = within(lane, LAT_OWN)
    r_of = (lane >= SEG).astype(jnp.int32) + (lane >= 2 * SEG).astype(jnp.int32)
    lon = lane - SEG * r_of
    sides = []
    for lat_step, share in ((-1, place.left["lat"]), (1, place.right["lat"])):
        before, same, after = (slots[slot_at(lon_step, lat_step), 0:8] for lon_step in (-1, 0, 1))
        side = jnp.where(within(lon, LON_OWN), same, 0.0)
        side = side + jnp.where(within(lon, 2), pltpu.roll(before, 128 - LON_OWN, 1), 0.0)
        side = side + jnp.where((lon >= LON_OWN) & (lon < LON_OWN + 2), pltpu.roll(after, LON_OWN, 1), 0.0)
        sides.append(side * share)
    blank = jnp.zeros((56, 128), jnp.float32)
    from_lat = []
    for g in range(4):
        head = jnp.where(within(row, 2), rolled(sides[0], 2 - 2 * g, 0), 0.0)
        tail = jnp.where(row < 2, rolled(sides[1], -2 * g, 0), 0.0)
        from_lat.append(jnp.concatenate([head, blank, tail, blank], axis=0).T)
    left = [slots[slot_at(-1, 0), at : at + 8] for at in (0, 8)]
    right = [slots[slot_at(1, 0), at : at + 8] for at in (0, 8)]
    for r in range(3):
        for g in range(4):
            index = 2 * r + g // 2
            shift = 66 if g % 2 else 2
            to = 2 * (index % 4)
            head = jnp.where(within(row, 2) & own_lane, pltpu.roll(rolled(left[index // 4], 2 - to, 0), shift, 1), 0.0)
            tail = jnp.where((row < 2) & own_lane, pltpu.roll(rolled(right[index // 4], -to, 0), shift, 1), 0.0)
            seg = tiles[r, g] + from_lat[g][r * SEG : (r + 1) * SEG]
            merged[r, g] = jnp.concatenate([seg[0:8] + head, seg[8:32], seg[32:40] + tail], axis=0)
    total = slots[0, 8:16]
    for j in range(1, slots.shape[0]):
        total = total + slots[j, 8:16]
    lines[...] = total
    low = lax.broadcasted_iota(jnp.int32, (SEG, 128), 1) < LAT_OWN

    def message(r, g):
        data = jnp.where(low, pltpu.roll(merged[r, g], 126, 1), pltpu.roll(merged[r, g + 1], 62, 1))
        return jnp.concatenate([data[:32], jnp.where(row < 4, data[32:], total)], axis=0)

    first[...], second[...] = place.messages("tm", message(0, 0), message(2, 2))


def join_kernel(tiles, got_first, got_second, joined, first, second):
    place = Place()
    lower = lax.broadcasted_iota(jnp.int32, (8, 128), 0) < 4
    for r in range(3):
        for g in range(4):
            left, right = place.received("lon", got_first[r, g // 2], got_second[r, g // 2])
            if g % 2:
                left, right = pltpu.roll(left, 4, 0), pltpu.roll(right, 4, 0)
            joined[r, g, 0:8] = tiles[r, g, 0:8] + jnp.where(lower, left, 0.0)
            joined[r, g, 8:32] = tiles[r, g, 8:32]
            joined[r, g, 32:40] = tiles[r, g, 32:40] + jnp.where(lower, right, 0.0)
    lane = lax.broadcasted_iota(jnp.int32, (SEG, 128), 1)

    def packed(r):
        rest = pltpu.roll(joined[r, 0], 64, 1)
        for g in range(1, 4):
            rest = jnp.where(lane < 4 * g, rest, pltpu.roll(joined[r, g], 64 + 4 * g, 1))
        return [jnp.where(lane < 64, joined[r, g], pltpu.roll(joined[r, g + 1], 64, 1)) for g in (0, 2)] + [rest]

    for i, (low_side, high_side) in enumerate(zip(packed(0), packed(2))):
        first[i], second[i] = place.messages("tm", low_side, high_side)


def turned_rows(tiles, g, left=0.0, right=0.0):
    parts = [tiles[0, g] + left, tiles[1, g], tiles[2, g] + right, jnp.zeros((8, 128), jnp.float32)]
    return jnp.concatenate(parts, axis=0).T


def turn_kernel(tiles, got_first, got_second, rows, first, second):
    place = Place()
    lane = lax.broadcasted_iota(jnp.int32, (SEG, 128), 1)
    sides = [place.received("tm", got_first[i], got_second[i]) for i in range(3)]

    def unpacked(g, side):
        main = rolled(sides[g // 2][side], -64 * (g % 2), 1)
        rest = rolled(sides[2][side], 64 - 4 * g, 1)
        return jnp.where(lane < 64, main, jnp.where(lane < LAT_OWN + 4, rest, 0.0))

    for g in range(4):
        block = turned_rows(tiles, g, unpacked(g, 0), unpacked(g, 1))
        lanes = slice(g * 128, (g + 1) * 128)
        rows[:, lanes] = block[:ROWS]
        first[:, lanes], second[:, lanes] = place.messages("lat", block[0:8], block[64:72])


def embed_kernel(own_both, tiles, first, second):
    place = Place()
    pair = lax.broadcasted_iota(jnp.int32, (8, 128), 0) // 2
    heads, tails = [None] * 4, [None] * 4
    for t in range(12):
        for k in range(2):
            if 2 <= t < T_OWN + 2:
                own = jnp.concatenate([own_both[k, t - 2], jnp.zeros((LON_OWN, 128 - LAT_OWN), jnp.float32)], axis=1)
                own = jnp.concatenate([own, jnp.zeros((SEG - LON_OWN, 128), jnp.float32)], axis=0)
                seg = pltpu.roll(pltpu.roll(own, 2, 0), 2, 1)
                at, tile = 2 * (t % 2) + k, (t - 2) // 2
                head, tail = rolled(seg[0:8], 2 * at - 2, 0), rolled(seg[32:40], 2 * at, 0)
                heads[tile] = head if at == 0 else jnp.where(pair == at, head, heads[tile])
                tails[tile] = tail if at == 0 else jnp.where(pair == at, tail, tails[tile])
            else:
                seg = jnp.zeros((SEG, 128), jnp.float32)
            tiles[k, t // 4, t % 4] = seg
    for tile in range(4):
        first[tile], second[tile] = place.messages("lon", heads[tile], tails[tile])


def embed_join_kernel(tiles, got_first, got_second, _, joined, first, second):
    place = Place()
    row = lax.broadcasted_iota(jnp.int32, (8, 128), 0)
    for k in range(2):
        for t in range(12):
            r, g = t // 4, t % 4
            if 2 <= t < T_OWN + 2:
                at, tile = 2 * (t % 2) + k, (t - 2) // 2
                left, right = place.received("lon", got_first[tile], got_second[tile])
                left, right = rolled(left, -2 * at, 0), rolled(right, 2 - 2 * at, 0)
                joined[k, r, g, 0:8] = tiles[k, r, g, 0:8] + jnp.where(row < 2, left, 0.0)
                joined[k, r, g, 8:32] = tiles[k, r, g, 8:32]
                joined[k, r, g, 32:40] = tiles[k, r, g, 32:40] + jnp.where((row >= 2) & (row < 4), right, 0.0)
            else:
                joined[k, r, g] = tiles[k, r, g]
    low = lax.broadcasted_iota(jnp.int32, (SEG, 128), 1) < LAT_OWN

    def beside(r, g):
        return jnp.where(low, pltpu.roll(joined[0, r, g], 126, 1), pltpu.roll(joined[1, r, g], 62, 1))

    for i in range(2):
        first[i], second[i] = place.messages("tm", beside(0, 2 + i), beside(2, i))


def embed_turn_kernel(tiles, got_first, got_second, rows, first, second):
    place = Place()
    lane = lax.broadcasted_iota(jnp.int32, (SEG, 128), 1)
    own = (lane >= 2) & (lane < LAT_OWN + 2)
    row = lax.broadcasted_iota(jnp.int32, (8, 128), 0)
    for g in range(4):
        lanes = slice(g * 128, (g + 1) * 128)
        left, right = place.received("tm", got_first[g % 2], got_second[g % 2])
        blocks = []
        for k in range(2):
            shift = 66 if k else 2
            if g < 2:
                block = turned_rows(tiles.at[k], g, left=jnp.where(own, pltpu.roll(left, shift, 1), 0.0))
            else:
                block = turned_rows(tiles.at[k], g, right=jnp.where(own, pltpu.roll(right, shift, 1), 0.0))
            rows[k, :, lanes] = block[:ROWS]
            blocks.append(block)
        head = jnp.where(row < 4, blocks[0][0:8], pltpu.roll(blocks[1][0:8], 2, 0))
        tail = jnp.where(row < 2, blocks[0][64:72], pltpu.roll(blocks[1][64:72], 2, 0))
        first[:, lanes], second[:, lanes] = place.messages("lat", head, tail)


def ready_kernel(_, *refs):
    for source, target in zip(refs[:4], refs[4:]):
        for g in range(4):
            turned = jnp.concatenate([source[:, g * 128 : (g + 1) * 128], jnp.zeros((128 - ROWS, 128), jnp.float32)], axis=0).T
            turned = pltpu.roll(turned, 126, 1)
            for r in range(3):
                t = 4 * r + g - 2
                if 0 <= t < T_OWN:
                    target[t] = pltpu.roll(turned[r * SEG : (r + 1) * SEG], SEG - 2, 0)[:LON_OWN]


def last_kernel(tiles, got_first, got_second, lines, got_lines, residual, scaled, image, image_scaled, step_out, residual_out):
    place = Place()
    total = lines[...] + got_lines[...] + got_first[32:40] + got_second[32:40]
    norm, curvature, image_norm, image_curvature = (jnp.sum(total[i : i + 1], axis=1, keepdims=True) for i in range(4, 8))
    step_size = norm / curvature
    next_norm = step_size * step_size * image_norm - norm
    ratio = next_norm / norm
    next_curvature = curvature - 2.0 * step_size * image_norm + step_size * step_size * image_curvature
    step_next = next_norm / (next_curvature - ratio * next_norm / step_size)
    left, right = place.received("tm", got_first[...], got_second[...])
    for t in range(T_OWN):
        merged = pltpu.roll(tiles[(t + 2) // 4, (t + 2) % 4], 126, 1)
        if t in (0, 1, T_OWN - 2, T_OWN - 1):
            merged = merged + rolled(left if t < 2 else right, 64 * (t % 2), 1)
        merged = pltpu.roll(merged, SEG - 2, 0)[:LON_OWN]
        s, y = scaled[t], image[t]
        step_out[t] = (step_size * s + step_next * (s - step_size * image_scaled[t] + ratio * s))[:, :LAT_OWN]
        left_over = residual[t] - step_size * y - step_next * (y - step_size * merged + ratio * y)
        residual_out[t] = left_over[:, :LAT_OWN]


def matchings(count):
    return [(i, (((i + 1) ^ 1) - 1) % count) for i in range(count)], [(i, i ^ 1) for i in range(count)]


def swap(first, second, axis):
    first_pairs, second_pairs = matchings(lax.axis_size(axis))
    return lax.ppermute(first, axis, first_pairs), lax.ppermute(second, axis, second_pairs)


def shaped(*shape):
    return jax.ShapeDtypeStruct(shape, jnp.float32)


def call(kernel, out_shape, name, *args, scratch=(), far=(), limit=24):
    vmem = pl.BlockSpec(memory_space=pltpu.VMEM)
    hbm = pl.BlockSpec(memory_space=pltpu.HBM)
    return pl.pallas_call(
        kernel,
        in_specs=[hbm if i in far else vmem for i in range(len(args))],
        out_specs=[vmem] * len(out_shape),
        out_shape=out_shape,
        scratch_shapes=scratch,
        compiler_params=pltpu.CompilerParams(vmem_limit_bytes=int(limit * 1024) * 1024),
        cost_estimate=pl.CostEstimate(flops=10**9, bytes_accessed=20 * 10**6, transcendentals=0),
        name=name,
    )(*args)


LON_MESSAGE, TM_MESSAGE, LAT_MESSAGE = (3, 2, 8, 128), (3, SEG, 128), (8, LANES)
TILES = (3, 4, SEG, 128)
VECTOR = (ROWS, LANES)
MID_SCRATCH, EDGE_SCRATCH = ([pltpu.VMEM((4 * n, 384), jnp.float32)] * m for n, m in ((CHUNK, 4), (EDGE_CELLS, 2)))
LOAD_LIMIT = 42
MID, ENDS = ((HOURS, n, LON_CELLS) for n in (MID_CELLS, EDGE_CELLS))


def exchange(tiles, first, second):
    first, second = swap(first, second, "lon")
    tiles, first, second = call(
        join_kernel, (shaped(*TILES), shaped(*TM_MESSAGE), shaped(*TM_MESSAGE)), "join", tiles, first, second
    )
    first, second = swap(first, second, "tm")
    rows, first, second = call(
        turn_kernel, (shaped(*VECTOR), shaped(*LAT_MESSAGE), shaped(*LAT_MESSAGE)), "turn", tiles, first, second
    )
    return rows, *swap(first, second, "lat")


def fold_and_sum(tiles, slots, lines_shape):
    slots = lax.all_to_all(slots, ("lon", "lat"), 0, 0, tiled=True)
    message = shaped(SEG, 128)
    tiles, first, second, lines = call(
        collect_kernel, (shaped(*TILES), message, message, lines_shape), "collect", tiles, slots
    )
    first, second = swap(first, second, "tm")
    count = lax.axis_size("tm")
    return tiles, first, second, lines, lax.ppermute(lines, "tm", [(i, (i + 2) % count) for i in range(count)])


def expand(coefficients, inverse_diag, offset, precip):
    tiles, message = shaped(2, *TILES), shaped(4, 8, 128)
    tiles_here, first, second = call(
        embed_kernel, (tiles, message, message), "embed", jnp.stack([coefficients, inverse_diag])
    )
    cells = call(
        load_kernel, (shaped(*MID), shaped(*MID), shaped(*ENDS), shaped(*ENDS)), "load", first, offset, precip,
        scratch=[pltpu.SemaphoreType.DMA((6,))], far=(1, 2), limit=LOAD_LIMIT,
    )
    first, second = swap(first, second, "lon")
    message = shaped(2, SEG, 128)
    tiles_here, first, second = call(embed_join_kernel, (tiles, message, message), "embed_join", tiles_here, first, second, cells[2])
    first, second = swap(first, second, "tm")
    shapes = (shaped(2, *VECTOR), shaped(*LAT_MESSAGE), shaped(*LAT_MESSAGE))
    both, first, second = call(embed_turn_kernel, shapes, "embed_turn", tiles_here, first, second)
    return both, *swap(first, second, "lat"), cells


def per_device(precip, offset, coefficients, inverse_diag):
    lat_total = LAT_CELLS * lax.axis_size("lat")
    lat_index = (lax.axis_index("lat") * LAT_CELLS + jnp.arange(LAT_CELLS, dtype=jnp.int32)).astype(jnp.float32)
    area = jnp.cos((90.0 - (lat_index + 0.5) * 180.0 / lat_total) * (jnp.pi / 180.0))
    area = jnp.broadcast_to(area[:, None], (LAT_CELLS, LON_CELLS))
    mid_tabs, edge_tabs = tables()
    ends = (shaped(*TILES), shaped(*LON_MESSAGE), shaped(*LON_MESSAGE))
    vector = shaped(*VECTOR)

    both, *got, cells = expand(coefficients.transpose(0, 2, 1), inverse_diag.transpose(0, 2, 1), offset, precip)
    weight, total = call(
        start_middle_kernel, (shaped(*MID), vector), "start_middle", both, middle(area), *cells[:2], *mid_tabs, scratch=MID_SCRATCH
    )
    edge_weight, diag, *sent = call(
        start_kernel, (shaped(*ENDS), vector, *ends), "start", both, *got, total, edges(area), *cells[2:],
        *edge_tabs, scratch=EDGE_SCRATCH,
    )

    def hessian(again, rows, got, outs, *more):
        total, = call(
            functools.partial(hessian_middle_kernel, again=again), (vector,), "hessian_middle", rows, diag, weight, *mid_tabs,
            scratch=MID_SCRATCH,
        )
        return call(
            functools.partial(hessian_kernel, again=again), (vector, vector, *outs), "hessian", rows, *got, total, diag,
            edge_weight, *edge_tabs, *more, scratch=EDGE_SCRATCH,
        )

    lines = shaped(8, 128)
    rows, *got = exchange(*sent)
    residual, scaled, *sent, sums = hessian(False, rows, got, (*ends, lines))
    slots = shaped(lax.axis_size("lon") * lax.axis_size("lat"), 16, 128)
    rows, *got = exchange(*sent)
    image, image_scaled, tiles, slots = hessian(True, rows, got, (ends[0], slots), sums)
    out = shaped(T_OWN, LON_OWN, LAT_OWN)
    folded = fold_and_sum(tiles, slots, lines)
    ready = call(
        ready_kernel, (shaped(T_OWN, LON_OWN, 128),) * 4, "ready", folded[3], residual, scaled, image, image_scaled
    )
    outs = call(last_kernel, (out, out), "last", *folded, *ready)
    return tuple(v.transpose(0, 2, 1) for v in outs)


def solution(mesh):
    return jax.shard_map(
        per_device, mesh=mesh, in_specs=(P(*SPLIT),) * 4, out_specs=(P(*SPLIT),) * 2, check_vma=False
    )
```

```python
import functools

import jax
import jax.numpy as jnp
import numpy as np
from jax import lax
from jax.experimental import pallas as pl
from jax.experimental.pallas import tpu as pltpu
from jax.sharding import PartitionSpec as P

SPLIT = ("tm", "lat", "lon")
tweedie_power = 1.6
smooth = 0.5

ROWS, LANES, SEG, LAT_OWN, LON_OWN, T_OWN = 80, 512, 40, 64, 32, 8
HOURS, LAT_CELLS, LON_CELLS = 32, 256, 128
EDGE, CHUNK = 16, 112
MID_CELLS, EDGE_CELLS = LAT_CELLS - 2 * EDGE, 2 * EDGE


def spline(offsets):
    distance = np.abs(offsets)
    near_part = (4.0 - 6.0 * distance**2 + 3.0 * distance**3) / 6.0
    far_part = np.maximum(2.0 - distance, 0.0) ** 3 / 6.0
    return np.where(distance < 1.0, near_part, far_part)


def table(cell_count, knot_count):
    cell_pos = np.arange(cell_count, dtype=np.float64)[:, None]
    knot_pos = np.arange(knot_count + 4, dtype=np.float64)[None, :] - 2.0
    return spline((cell_pos - 4.0 * knot_pos - 1.5) / 4.0)


def halves(values):
    values = jnp.asarray(values, jnp.float32)
    high = values.astype(jnp.bfloat16)
    return high, (values - high.astype(jnp.float32)).astype(jnp.bfloat16)


def middle(cells, axis=0):
    return lax.slice_in_dim(cells, EDGE, LAT_CELLS - EDGE, axis=axis)


def edges(cells, axis=0):
    ends = (lax.slice_in_dim(cells, at, at + EDGE, axis=axis) for at in (0, LAT_CELLS - EDGE))
    return jnp.concatenate(list(ends), axis=axis)


def tables():
    lat = np.zeros((LAT_CELLS, ROWS))
    lat[:, : LAT_OWN + 4] = table(LAT_CELLS, LAT_OWN)
    high, low = halves(lat)
    lat_tables = []
    for part in (middle, edges):
        up = jnp.concatenate([part(high), part(low), part(high)], axis=1)
        cells = CHUNK if part is middle else EDGE_CELLS
        down = [p.reshape(-1, cells, ROWS).transpose(0, 2, 1) for p in (part(high), part(low))]
        lat_tables += [up, jnp.concatenate([down[0], down[1], down[0]], axis=2)]
    lon = np.zeros((128, 3 * LON_CELLS))
    for r in range(3):
        lon[r * SEG : r * SEG + LON_OWN + 4, r * LON_CELLS : (r + 1) * LON_CELLS] = table(LON_CELLS, LON_OWN).T
    high, low = halves(lon)
    lon_up = jnp.concatenate([high, high, low], axis=0)
    lon_down = jnp.concatenate([high.T, low.T], axis=1)
    return lat_tables[:2] + [lon_up, lon_down], lat_tables[2:] + [lon_up, lon_down]


def hour_factors():
    near, far = ([float(spline(np.float64(x))) for x in xs] for xs in ((0.125, 0.875, 0.375, 0.625), (1.125, 1.875, 1.375, 1.625)))
    outer = ((far[0] + far[1]) / 2, (far[0] - far[1]) / 2, (far[2] + far[3]) / 2, (far[2] - far[3]) / 2)
    inner = ((near[0] + near[1]) / 2, (near[0] - near[1]) / 2, (near[2] + near[3]) / 2, (near[2] - near[3]) / 2)
    return outer, inner


class Place:
    def __init__(self):
        index = {axis: lax.axis_index(axis) for axis in SPLIT}
        self.even = {axis: index[axis] % 2 == 0 for axis in SPLIT}
        self.left = {axis: jnp.where(index[axis] > 0, 1.0, 0.0) for axis in SPLIT}
        self.right = {axis: jnp.where(index[axis] < lax.axis_size(axis) - 1, 1.0, 0.0) for axis in SPLIT}

    def messages(self, axis, to_left, to_right):
        return jnp.where(self.even[axis], to_left, to_right), jnp.where(self.even[axis], to_right, to_left)

    def received(self, axis, first, second):
        left, right = jnp.where(self.even[axis], first, second), jnp.where(self.even[axis], second, first)
        return (left, right) if axis == "lon" else (left * self.left[axis], right * self.right[axis])


def split(values):
    high = values.astype(jnp.bfloat16)
    return high, (values - high.astype(jnp.float32)).astype(jnp.bfloat16)


def dot(left, right):
    return jnp.dot(left, right, preferred_element_type=jnp.float32)


def lane_places():
    lane = lax.broadcasted_iota(jnp.int32, (ROWS, 128), 1)
    r = (lane >= SEG).astype(jnp.int32) + (lane >= 2 * SEG).astype(jnp.int32)
    return r, lane - SEG * r, lax.broadcasted_iota(jnp.int32, (ROWS, 128), 0)


def within(place, count):
    return (place >= 2) & (place < count + 2)


def group(values, g):
    return values[:, g * 128 : (g + 1) * 128]


def penalty(values, place):
    r, lon, row = lane_places()
    own_row, own_lon = within(row, LAT_OWN), within(lon, LON_OWN)
    row_share = jnp.where(
        own_row, 1.0, jnp.where(row == 1, 1.0 - place.left["lat"], jnp.where(row == LAT_OWN + 2, 1.0 - place.right["lat"], 0.0))
    )
    parts = [group(values, g) for g in range(4)]

    def along_t(v):
        before = [pltpu.roll(v[3], SEG, 1), v[0], v[1], v[2]]
        after = [v[1], v[2], v[3], pltpu.roll(v[0], 128 - SEG, 1)]
        return [b - 2.0 * m + a for b, m, a in zip(before, v, after)]

    t_second = along_t(parts)
    t_shared = []
    summed = []
    for g in range(4):
        t = 4 * r + g
        own_t = within(t, T_OWN)
        share = jnp.where(own_t, 1.0, jnp.where(t == 1, 1.0 - place.left["tm"], jnp.where(t == T_OWN + 2, 1.0 - place.right["tm"], 0.0)))
        t_shared.append(jnp.where(own_row & own_lon, share, 0.0) * t_second[g])
        v = parts[g]
        second = pltpu.roll(v, 1, 0) - 2.0 * v + pltpu.roll(v, ROWS - 1, 0)
        second = jnp.where(own_t & own_lon, row_share, 0.0) * second
        total = pltpu.roll(second, 1, 0) - 2.0 * second + pltpu.roll(second, ROWS - 1, 0)
        second = pltpu.roll(v, 1, 1) - 2.0 * v + pltpu.roll(v, 127, 1)
        second = jnp.where(own_t & own_lon & own_row, second, 0.0)
        summed.append(total + pltpu.roll(second, 1, 1) - 2.0 * second + pltpu.roll(second, 127, 1))
    return [smooth * (a + b) for a, b in zip(summed, along_t(t_shared))]


def lane_sum(parts):
    return jnp.sum(parts[0] + parts[1] + parts[2] + parts[3], axis=0, keepdims=True)


def own_lane_sum(values):
    r, lon, row = lane_places()
    inside = within(row, LAT_OWN) & within(lon, LON_OWN)
    return lane_sum([jnp.where(inside & within(4 * r + g, T_OWN), group(values, g), 0.0) for g in range(4)])


def merge_rows(values, got_first, got_second, place):
    keep = lax.broadcasted_iota(jnp.int32, (8, LANES), 0) < 4
    left, right = place.received("lat", got_first, got_second)
    return jnp.concatenate(
        [
            values[0:8] + jnp.where(keep, left, 0.0),
            values[8:64],
            values[64:72] + jnp.where(keep, right, 0.0),
            values[72:80],
        ],
        axis=0,
    )


def expand_cells(parts, lat_up, lon_up, up):
    expanded = dot(lat_up, parts)
    high, low = split(jnp.concatenate([group(expanded, g) for g in range(4)], axis=0))
    up[...] = dot(jnp.concatenate([high, low, high], axis=1), lon_up[...])


def cells_tile(w_of, first_row, start, cells, up, down):
    outer, inner = hour_factors()
    rows = pl.ds(first_row + start, 8)

    def knot(t):
        return up[pl.ds((t % 4) * cells + start, 8), (t // 4) * 128 : (t // 4 + 1) * 128]

    back = [None] * 12

    def add(t, value):
        back[t] = value if back[t] is None else back[t] + value

    x = [knot(0), knot(1), knot(2), None]
    for j in range(9):
        x[3] = knot(j + 3)
        edge_sum, edge_diff, mid_sum, mid_diff = x[0] + x[3], x[0] - x[3], x[1] + x[2], x[1] - x[2]
        sides = []
        for pair, (late, early) in enumerate(((2, 1), (3, 0))):
            even = outer[2 * pair] * edge_sum + inner[2 * pair] * mid_sum
            uneven = outer[2 * pair + 1] * edge_diff + inner[2 * pair + 1] * mid_diff
            below = w_of(4 * (j - 1) + late, rows, even + uneven) if j > 0 else None
            above = w_of(4 * j + early, rows, even - uneven) if j < 8 else None
            if below is None:
                sides.append((above, -above))
            elif above is None:
                sides.append((below, below))
            else:
                sides.append((below + above, below - above))
        (both0, differ0), (both1, differ1) = sides
        edge_even, edge_odd = outer[0] * both0 + outer[2] * both1, outer[1] * differ0 + outer[3] * differ1
        mid_even, mid_odd = inner[0] * both0 + inner[2] * both1, inner[1] * differ0 + inner[3] * differ1
        add(j, edge_even + edge_odd)
        add(j + 1, mid_even + mid_odd)
        add(j + 2, mid_even - mid_odd)
        add(j + 3, edge_even - edge_odd)
        for t in (j,) if j < 8 else (8, 9, 10, 11):
            down[pl.ds((t % 4) * cells + start, 8), (t // 4) * 128 : (t // 4 + 1) * 128] = back[t]
        x = [x[1], x[2], x[3], None]


def fold_cells(down, cells, lat_down, lon_down):
    high, low = split(down[...])
    both = dot(high, lon_down[...])
    narrow = both[:, :128] + both[:, 128:] + dot(low, lon_down[:, :128])
    narrow = jnp.concatenate([narrow[g * cells : (g + 1) * cells] for g in range(4)], axis=1)
    high, low = split(narrow)
    return dot(lat_down, jnp.concatenate([high, high, low], axis=0))


def apply_cells(values, w_of, lat_up, lat_down, lon_up, lon_down, *scratch):
    high, low = split(values)
    parts = jnp.concatenate([high, high, low], axis=0)
    chunks, _, _ = lat_down.shape
    cells = lat_up.shape[0] // chunks
    buffers = scratch[:2], scratch[2:]
    expand_cells(parts, lat_up[0:cells], lon_up, buffers[0][0])
    total = None
    for chunk in range(chunks):
        up, down = buffers[chunk % 2]
        if chunk + 1 < chunks:
            expand_cells(parts, lat_up[(chunk + 1) * cells : (chunk + 2) * cells], lon_up, buffers[(chunk + 1) % 2][0])
        for start in range(0, cells, 8):
            cells_tile(w_of, chunk * cells, start, cells, up, down)
        part = fold_cells(down, cells, lat_down[chunk], lon_down)
        total = part if total is None else total + part
    return total


def finish(total, values, place):
    extra = penalty(values, place)
    sums = [group(total, g) + extra[g] for g in range(4)]
    turned = [jnp.concatenate([part, jnp.zeros((128 - ROWS, 128), jnp.float32)], axis=0).T for part in sums]
    return sums, [[turned[g][r * SEG : (r + 1) * SEG] for g in range(4)] for r in range(3)]


def rolled(values, amount, axis):
    amount %= values.shape[axis]
    return pltpu.roll(values, amount, axis) if amount else values


def pack_lanes(parts):
    lane = lax.broadcasted_iota(jnp.int32, parts[0].shape, 1)
    rest = pltpu.roll(parts[0], 64, 1)
    for i in range(1, len(parts)):
        rest = jnp.where(lane < 4 * i, rest, pltpu.roll(parts[i], 64 + 4 * i, 1))
    pairs = [jnp.where(lane < 64, parts[i], pltpu.roll(parts[i + 1], 64, 1)) for i in range(0, len(parts), 2)]
    return pairs + [rest]


def unpack_lanes(packs, i):
    lane = lax.broadcasted_iota(jnp.int32, packs[0].shape, 1)
    main, rest = rolled(packs[i // 2], -64 * (i % 2), 1), rolled(packs[-1], 64 - 4 * i, 1)
    return jnp.where(lane < 64, main, jnp.where(lane < LAT_OWN + 4, rest, 0.0))


def write_ends(segs, place, tiles, first, second):
    lower = lax.broadcasted_iota(jnp.int32, (8, 128), 0) < 4
    sides = []
    for at in (0, 32):
        parts = []
        for r in range(3):
            for h in range(2):
                pair = (segs[r][2 * h + i][at : at + 8] for i in range(2))
                parts.append(jnp.where(lower, next(pair), pltpu.roll(next(pair), 4, 0)))
        sides.append(pack_lanes(parts))
    for r in range(3):
        for g in range(4):
            tiles[r, g] = segs[r][g]
    for i, pair in enumerate(zip(*sides)):
        first[i], second[i] = place.messages("lon", *pair)


def start_of(area, offset, precip, weight):
    def w_of(hour, rows, value):
        linear = offset[hour, rows, :] + value
        here = area[rows, :]
        w = here * jnp.exp((2.0 - tweedie_power) * linear)
        weight[hour, rows, :] = w
        return w - here * precip[hour, rows, :] * jnp.exp((1.0 - tweedie_power) * linear)

    return w_of


def load_kernel(_, offset_far, precip_far, offset, precip, offset_edges, precip_edges, arrived):
    copies = []

    def bring(source, source_at, target, target_at, count):
        source, target = source.at[:, pl.ds(source_at, count), :], target.at[:, pl.ds(target_at, count), :]
        copies.append(pltpu.make_async_copy(source, target, arrived.at[len(copies)]))

    for source, target, ends in ((offset_far, offset, offset_edges), (precip_far, precip, precip_edges)):
        bring(source, EDGE, target, 0, MID_CELLS)
        bring(source, 0, ends, 0, EDGE)
        bring(source, LAT_CELLS - EDGE, ends, EDGE, EDGE)
    for copy in copies:
        copy.start()
    for copy in copies:
        copy.wait()


def start_middle_kernel(both, area, offset, precip, lat_up, lat_down, lon_up, lon_down, weight, total, *scratch):
    w_of = start_of(area, offset, precip, weight)
    total[...] = apply_cells(both[0], w_of, lat_up, lat_down, lon_up, lon_down, *scratch)


def start_kernel(both, got_first, got_second, total, area, offset, precip, lat_up, lat_down, lon_up, lon_down,
                 weight, diag, tiles, first, second, *scratch):
    place = Place()
    row = lax.broadcasted_iota(jnp.int32, (8, LANES), 0)
    left, right = place.received("lat", got_first[...], got_second[...])

    def with_halo(own, left, right):
        head, tail = own[0:8] + jnp.where(row < 2, left, 0.0), own[64:72] + jnp.where((row >= 2) & (row < 4), right, 0.0)
        return jnp.concatenate([head, own[8:64], tail, own[72:80]], axis=0)

    values = with_halo(both[0], left, right)
    diag[...] = with_halo(both[1], pltpu.roll(left, 6, 0), pltpu.roll(right, 6, 0))
    w_of = start_of(area, offset, precip, weight)
    part = apply_cells(values, w_of, lat_up, lat_down, lon_up, lon_down, *scratch)
    _, segs = finish(total[...] + part, values, place)
    write_ends(segs, place, tiles, first, second)


def weigh(weight):
    return lambda hour, rows, value: weight[hour, rows, :] * value


def hessian_middle_kernel(partial_rows, diag, weight, lat_up, lat_down, lon_up, lon_down, total, *scratch, again):
    here = partial_rows[...] if again else -partial_rows[...]
    total[...] = apply_cells(diag[...] * here, weigh(weight), lat_up, lat_down, lon_up, lon_down, *scratch)


def hessian_kernel(partial_rows, got_first, got_second, total, diag, weight, lat_up, lat_down, lon_up, lon_down, *refs, again):
    if again:
        before, residual, scaled, tiles, slots, *scratch = refs
    else:
        residual, scaled, tiles, first, second, sums, *scratch = refs
    place = Place()
    merged = merge_rows(partial_rows[...], got_first[...], got_second[...], place)
    here = merged if again else -merged
    residual[...] = here
    values = diag[...] * here
    scaled[...] = values
    part = apply_cells(values, weigh(weight), lat_up, lat_down, lon_up, lon_down, *scratch)
    image, segs = finish(total[...] + part, values, place)
    lines = [own_lane_sum(here * values), lane_sum([image[g] * group(values, g) for g in range(4)])]
    if again:
        for r in range(3):
            for g in range(4):
                tiles[r, g] = segs[r][g]
        lines = jnp.concatenate([jnp.zeros((4, 128), jnp.float32), before[0:2], *lines], axis=0)
        write_slots(image, segs, lines, slots)
    else:
        write_ends(segs, place, tiles, first, second)
        sums[...] = jnp.concatenate(lines + [jnp.zeros((6, 128), jnp.float32)], axis=0)


def slot_at(lon_step, lat_step):
    lon_count, lat_count = lax.axis_size("lon"), lax.axis_size("lat")
    lon = lax.rem(lax.axis_index("lon") + (lon_count + lon_step), lon_count)
    return lon * lat_count + lax.rem(lax.axis_index("lat") + (lat_count + lat_step), lat_count)


def row_of(shape=(8, 128)):
    return lax.broadcasted_iota(jnp.int32, shape, 0)


def write_slots(sums, segs, lines, slots):
    row = row_of()
    low = lax.broadcasted_iota(jnp.int32, (8, 128), 1) < LAT_OWN
    for j in range(slots.shape[0]):
        slots[j, 0:8] = jnp.zeros((8, 128), jnp.float32)
        slots[j, 8:16] = lines
    for step, at, skip in ((-1, 0, 0), (1, 32, 2)):
        halves_of = [jnp.zeros((8, 128), jnp.float32), lines]
        for r in range(3):
            for h in range(2):
                index = 2 * r + h
                pair = jnp.where(
                    low, pltpu.roll(segs[r][2 * h][at : at + 8], 126, 1), pltpu.roll(segs[r][2 * h + 1][at : at + 8], 62, 1)
                )
                to = 2 * (index % 4)
                part = rolled(pair, to - skip, 0)
                halves_of[index // 4] = jnp.where((row >= to) & (row < to + 2), part, halves_of[index // 4])
        slot = slot_at(step, 0)
        slots[slot, 0:8] = halves_of[0]
        slots[slot, 8:16] = halves_of[1]
    for lat_step, at, skip in ((-1, 0, 0), (1, 64, 2)):
        content = jnp.zeros((8, 128), jnp.float32)
        for g in range(4):
            part = rolled(sums[g][at : at + 8], 2 * g - skip, 0)
            content = jnp.where((row >= 2 * g) & (row < 2 * g + 2), part, content)
        for lon_step in (-1, 0, 1):
            slots[slot_at(lon_step, lat_step), 0:8] = content


def collect_kernel(tiles, slots, merged, first, second, lines):
    place = Place()
    row = row_of()
    lane = lax.broadcasted_iota(jnp.int32, (8, 128), 1)
    own_lane = within(lane, LAT_OWN)
    r_of = (lane >= SEG).astype(jnp.int32) + (lane >= 2 * SEG).astype(jnp.int32)
    lon = lane - SEG * r_of
    sides = []
    for lat_step, share in ((-1, place.left["lat"]), (1, place.right["lat"])):
        before, same, after = (slots[slot_at(lon_step, lat_step), 0:8] for lon_step in (-1, 0, 1))
        side = jnp.where(within(lon, LON_OWN), same, 0.0)
        side = side + jnp.where(within(lon, 2), pltpu.roll(before, 128 - LON_OWN, 1), 0.0)
        side = side + jnp.where((lon >= LON_OWN) & (lon < LON_OWN + 2), pltpu.roll(after, LON_OWN, 1), 0.0)
        sides.append(side * share)
    blank = jnp.zeros((56, 128), jnp.float32)
    from_lat = []
    for g in range(4):
        head = jnp.where(within(row, 2), rolled(sides[0], 2 - 2 * g, 0), 0.0)
        tail = jnp.where(row < 2, rolled(sides[1], -2 * g, 0), 0.0)
        from_lat.append(jnp.concatenate([head, blank, tail, blank], axis=0).T)
    left = [slots[slot_at(-1, 0), at : at + 8] for at in (0, 8)]
    right = [slots[slot_at(1, 0), at : at + 8] for at in (0, 8)]
    for r in range(3):
        for g in range(4):
            index = 2 * r + g // 2
            shift = 66 if g % 2 else 2
            to = 2 * (index % 4)
            head = jnp.where(within(row, 2) & own_lane, pltpu.roll(rolled(left[index // 4], 2 - to, 0), shift, 1), 0.0)
            tail = jnp.where((row < 2) & own_lane, pltpu.roll(rolled(right[index // 4], -to, 0), shift, 1), 0.0)
            seg = tiles[r, g] + from_lat[g][r * SEG : (r + 1) * SEG]
            merged[r, g] = jnp.concatenate([seg[0:8] + head, seg[8:32], seg[32:40] + tail], axis=0)
    total = slots[0, 8:16]
    for j in range(1, slots.shape[0]):
        total = total + slots[j, 8:16]
    lines[...] = total
    low = lax.broadcasted_iota(jnp.int32, (SEG, 128), 1) < LAT_OWN

    def message(r, g):
        data = jnp.where(low, pltpu.roll(merged[r, g], 126, 1), pltpu.roll(merged[r, g + 1], 62, 1))
        return jnp.concatenate([data[:32], jnp.where(row < 4, data[32:], total)], axis=0)

    first[...], second[...] = place.messages("tm", message(0, 0), message(2, 2))


def join_kernel(tiles, got_first, got_second, joined, first, second):
    place = Place()
    lower = lax.broadcasted_iota(jnp.int32, (8, 128), 0) < 4
    lefts, rights = zip(*(place.received("lon", got_first[i], got_second[i]) for i in range(4)))
    for r in range(3):
        for h in range(2):
            pair_left, pair_right = unpack_lanes(lefts, 2 * r + h), unpack_lanes(rights, 2 * r + h)
            for g in (2 * h, 2 * h + 1):
                left, right = rolled(pair_left, 4 * (g % 2), 0), rolled(pair_right, 4 * (g % 2), 0)
                joined[r, g, 0:8] = tiles[r, g, 0:8] + jnp.where(lower, left, 0.0)
                joined[r, g, 8:32] = tiles[r, g, 8:32]
                joined[r, g, 32:40] = tiles[r, g, 32:40] + jnp.where(lower, right, 0.0)
    for i, pair in enumerate(zip(*(pack_lanes([joined[r, g] for g in range(4)]) for r in (0, 2)))):
        first[i], second[i] = place.messages("tm", *pair)


def turned_rows(tiles, g, left=0.0, right=0.0):
    parts = [tiles[0, g] + left, tiles[1, g], tiles[2, g] + right, jnp.zeros((8, 128), jnp.float32)]
    return jnp.concatenate(parts, axis=0).T


def turn_kernel(tiles, got_first, got_second, rows, first, second):
    place = Place()
    lefts, rights = zip(*(place.received("tm", got_first[i], got_second[i]) for i in range(3)))
    for g in range(4):
        block = turned_rows(tiles, g, unpack_lanes(lefts, g), unpack_lanes(rights, g))
        lanes = slice(g * 128, (g + 1) * 128)
        rows[:, lanes] = block[:ROWS]
        first[:, lanes], second[:, lanes] = place.messages("lat", block[0:8], block[64:72])


def embed_kernel(own_both, tiles, first, second):
    place = Place()
    pair = lax.broadcasted_iota(jnp.int32, (8, 128), 0) // 2
    heads, tails = [None] * 4, [None] * 4
    for t in range(12):
        for k in range(2):
            if 2 <= t < T_OWN + 2:
                own = jnp.concatenate([own_both[k, t - 2], jnp.zeros((LON_OWN, 128 - LAT_OWN), jnp.float32)], axis=1)
                own = jnp.concatenate([own, jnp.zeros((SEG - LON_OWN, 128), jnp.float32)], axis=0)
                seg = pltpu.roll(pltpu.roll(own, 2, 0), 2, 1)
                at, tile = 2 * (t % 2) + k, (t - 2) // 2
                head, tail = rolled(seg[0:8], 2 * at - 2, 0), rolled(seg[32:40], 2 * at, 0)
                heads[tile] = head if at == 0 else jnp.where(pair == at, head, heads[tile])
                tails[tile] = tail if at == 0 else jnp.where(pair == at, tail, tails[tile])
            else:
                seg = jnp.zeros((SEG, 128), jnp.float32)
            tiles[k, t // 4, t % 4] = seg
    for tile in range(4):
        first[tile], second[tile] = place.messages("lon", heads[tile], tails[tile])


def embed_join_kernel(tiles, got_first, got_second, _, joined, first, second):
    place = Place()
    row = lax.broadcasted_iota(jnp.int32, (8, 128), 0)
    for k in range(2):
        for t in range(12):
            r, g = t // 4, t % 4
            if 2 <= t < T_OWN + 2:
                at, tile = 2 * (t % 2) + k, (t - 2) // 2
                left, right = place.received("lon", got_first[tile], got_second[tile])
                left, right = rolled(left, -2 * at, 0), rolled(right, 2 - 2 * at, 0)
                joined[k, r, g, 0:8] = tiles[k, r, g, 0:8] + jnp.where(row < 2, left, 0.0)
                joined[k, r, g, 8:32] = tiles[k, r, g, 8:32]
                joined[k, r, g, 32:40] = tiles[k, r, g, 32:40] + jnp.where((row >= 2) & (row < 4), right, 0.0)
            else:
                joined[k, r, g] = tiles[k, r, g]
    low = lax.broadcasted_iota(jnp.int32, (SEG, 128), 1) < LAT_OWN

    def beside(r, g):
        return jnp.where(low, pltpu.roll(joined[0, r, g], 126, 1), pltpu.roll(joined[1, r, g], 62, 1))

    for i in range(2):
        first[i], second[i] = place.messages("tm", beside(0, 2 + i), beside(2, i))


def embed_turn_kernel(tiles, got_first, got_second, rows, first, second):
    place = Place()
    lane = lax.broadcasted_iota(jnp.int32, (SEG, 128), 1)
    own = (lane >= 2) & (lane < LAT_OWN + 2)
    row = lax.broadcasted_iota(jnp.int32, (8, 128), 0)
    for g in range(4):
        lanes = slice(g * 128, (g + 1) * 128)
        left, right = place.received("tm", got_first[g % 2], got_second[g % 2])
        blocks = []
        for k in range(2):
            shift = 66 if k else 2
            if g < 2:
                block = turned_rows(tiles.at[k], g, left=jnp.where(own, pltpu.roll(left, shift, 1), 0.0))
            else:
                block = turned_rows(tiles.at[k], g, right=jnp.where(own, pltpu.roll(right, shift, 1), 0.0))
            rows[k, :, lanes] = block[:ROWS]
            blocks.append(block)
        head = jnp.where(row < 4, blocks[0][0:8], pltpu.roll(blocks[1][0:8], 2, 0))
        tail = jnp.where(row < 2, blocks[0][64:72], pltpu.roll(blocks[1][64:72], 2, 0))
        first[:, lanes], second[:, lanes] = place.messages("lat", head, tail)


def ready_kernel(_, *refs):
    for source, target in zip(refs[:4], refs[4:]):
        for g in range(4):
            turned = jnp.concatenate([source[:, g * 128 : (g + 1) * 128], jnp.zeros((128 - ROWS, 128), jnp.float32)], axis=0).T
            turned = pltpu.roll(turned, 126, 1)
            for r in range(3):
                t = 4 * r + g - 2
                if 0 <= t < T_OWN:
                    target[t] = pltpu.roll(turned[r * SEG : (r + 1) * SEG], SEG - 2, 0)[:LON_OWN]


def last_kernel(tiles, got_first, got_second, lines, got_lines, residual, scaled, image, image_scaled, step_out, residual_out):
    place = Place()
    total = lines[...] + got_lines[...] + got_first[32:40] + got_second[32:40]
    norms, curvatures, image_norms, image_curvatures = (total[i : i + 1] for i in range(4, 8))

    def all_lanes(values):
        return jnp.sum(values, axis=1, keepdims=True)

    norm = all_lanes(norms)
    step_size = norm / all_lanes(curvatures)
    next_norm = all_lanes(norms + step_size * (step_size * image_norms - 2.0 * curvatures))
    next_curvature = all_lanes(curvatures + step_size * (step_size * image_curvatures - 2.0 * image_norms))
    ratio = next_norm / norm
    step_next = next_norm / (next_curvature - ratio * next_norm / step_size)
    left, right = place.received("tm", got_first[...], got_second[...])
    for t in range(T_OWN):
        merged = pltpu.roll(tiles[(t + 2) // 4, (t + 2) % 4], 126, 1)
        if t in (0, 1, T_OWN - 2, T_OWN - 1):
            merged = merged + rolled(left if t < 2 else right, 64 * (t % 2), 1)
        merged = pltpu.roll(merged, SEG - 2, 0)[:LON_OWN]
        s, y = scaled[t], image[t]
        step_out[t] = (step_size * s + step_next * (s - step_size * image_scaled[t] + ratio * s))[:, :LAT_OWN]
        left_over = residual[t] - step_size * y - step_next * (y - step_size * merged + ratio * y)
        residual_out[t] = left_over[:, :LAT_OWN]


def matchings(count):
    return [(i, (((i + 1) ^ 1) - 1) % count) for i in range(count)], [(i, i ^ 1) for i in range(count)]


def swap(first, second, axis):
    first_pairs, second_pairs = matchings(lax.axis_size(axis))
    return lax.ppermute(first, axis, first_pairs), lax.ppermute(second, axis, second_pairs)


def shaped(*shape):
    return jax.ShapeDtypeStruct(shape, jnp.float32)


def call(kernel, out_shape, name, *args, scratch=(), far=(), limit=24):
    vmem = pl.BlockSpec(memory_space=pltpu.VMEM)
    hbm = pl.BlockSpec(memory_space=pltpu.HBM)
    return pl.pallas_call(
        kernel,
        in_specs=[hbm if i in far else vmem for i in range(len(args))],
        out_specs=[vmem] * len(out_shape),
        out_shape=out_shape,
        scratch_shapes=scratch,
        compiler_params=pltpu.CompilerParams(vmem_limit_bytes=int(limit * 1024) * 1024),
        cost_estimate=pl.CostEstimate(flops=10**9, bytes_accessed=20 * 10**6, transcendentals=0),
        name=name,
    )(*args)


LON_MESSAGE, TM_MESSAGE, LAT_MESSAGE = (4, 8, 128), (3, SEG, 128), (8, LANES)
TILES = (3, 4, SEG, 128)
VECTOR = (ROWS, LANES)
MID_SCRATCH, EDGE_SCRATCH = ([pltpu.VMEM((4 * n, 384), jnp.float32)] * m for n, m in ((CHUNK, 4), (EDGE_CELLS, 2)))
LOAD_LIMIT = 42
MID, ENDS = ((HOURS, n, LON_CELLS) for n in (MID_CELLS, EDGE_CELLS))


def exchange(tiles, first, second):
    first, second = swap(first, second, "lon")
    tiles, first, second = call(
        join_kernel, (shaped(*TILES), shaped(*TM_MESSAGE), shaped(*TM_MESSAGE)), "join", tiles, first, second
    )
    first, second = swap(first, second, "tm")
    rows, first, second = call(
        turn_kernel, (shaped(*VECTOR), shaped(*LAT_MESSAGE), shaped(*LAT_MESSAGE)), "turn", tiles, first, second
    )
    return rows, *swap(first, second, "lat")


def fold_and_sum(tiles, slots, lines_shape):
    slots = lax.all_to_all(slots, ("lon", "lat"), 0, 0, tiled=True)
    message = shaped(SEG, 128)
    tiles, first, second, lines = call(
        collect_kernel, (shaped(*TILES), message, message, lines_shape), "collect", tiles, slots
    )
    first, second = swap(first, second, "tm")
    count = lax.axis_size("tm")
    got_lines = lax.ppermute(lines, "tm", [(i, (i + 2) % count) for i in range(count)])
    return tiles, first, second, lines, got_lines


def expand(coefficients, inverse_diag, offset, precip):
    tiles, message = shaped(2, *TILES), shaped(4, 8, 128)
    tiles_here, first, second = call(
        embed_kernel, (tiles, message, message), "embed", jnp.stack([coefficients, inverse_diag])
    )
    cells = call(
        load_kernel, (shaped(*MID), shaped(*MID), shaped(*ENDS), shaped(*ENDS)), "load", first, offset, precip,
        scratch=[pltpu.SemaphoreType.DMA((6,))], far=(1, 2), limit=LOAD_LIMIT,
    )
    first, second = swap(first, second, "lon")
    message = shaped(2, SEG, 128)
    tiles_here, first, second = call(embed_join_kernel, (tiles, message, message), "embed_join", tiles_here, first, second, cells[2])
    first, second = swap(first, second, "tm")
    shapes = (shaped(2, *VECTOR), shaped(*LAT_MESSAGE), shaped(*LAT_MESSAGE))
    both, first, second = call(embed_turn_kernel, shapes, "embed_turn", tiles_here, first, second)
    return both, *swap(first, second, "lat"), cells


def per_device(precip, offset, coefficients, inverse_diag):
    lat_total = LAT_CELLS * lax.axis_size("lat")
    lat_index = (lax.axis_index("lat") * LAT_CELLS + jnp.arange(LAT_CELLS, dtype=jnp.int32)).astype(jnp.float32)
    area = jnp.cos((90.0 - (lat_index + 0.5) * 180.0 / lat_total) * (jnp.pi / 180.0))
    area = jnp.broadcast_to(area[:, None], (LAT_CELLS, LON_CELLS))
    mid_tabs, edge_tabs = tables()
    ends = (shaped(*TILES), shaped(*LON_MESSAGE), shaped(*LON_MESSAGE))
    vector = shaped(*VECTOR)

    both, *got, cells = expand(coefficients.transpose(0, 2, 1), inverse_diag.transpose(0, 2, 1), offset, precip)
    weight, total = call(
        start_middle_kernel, (shaped(*MID), vector), "start_middle", both, middle(area), *cells[:2], *mid_tabs, scratch=MID_SCRATCH
    )
    edge_weight, diag, *sent = call(
        start_kernel, (shaped(*ENDS), vector, *ends), "start", both, *got, total, edges(area), *cells[2:],
        *edge_tabs, scratch=EDGE_SCRATCH,
    )

    def hessian(again, rows, got, outs, *more):
        total, = call(
            functools.partial(hessian_middle_kernel, again=again), (vector,), "hessian_middle", rows, diag, weight, *mid_tabs,
            scratch=MID_SCRATCH,
        )
        return call(
            functools.partial(hessian_kernel, again=again), (vector, vector, *outs), "hessian", rows, *got, total, diag,
            edge_weight, *edge_tabs, *more, scratch=EDGE_SCRATCH,
        )

    lines = shaped(8, 128)
    rows, *got = exchange(*sent)
    residual, scaled, *sent, sums = hessian(False, rows, got, (*ends, lines))
    slots = shaped(lax.axis_size("lon") * lax.axis_size("lat"), 16, 128)
    rows, *got = exchange(*sent)
    image, image_scaled, tiles, slots = hessian(True, rows, got, (ends[0], slots), sums)
    out = shaped(T_OWN, LON_OWN, LAT_OWN)
    folded = fold_and_sum(tiles, slots, lines)
    ready = call(
        ready_kernel, (shaped(T_OWN, LON_OWN, 128),) * 4, "ready", folded[3], residual, scaled, image, image_scaled
    )
    outs = call(last_kernel, (out, out), "last", *folded, *ready)
    return tuple(v.transpose(0, 2, 1) for v in outs)


def solution(mesh):
    return jax.shard_map(
        per_device, mesh=mesh, in_specs=(P(*SPLIT),) * 4, out_specs=(P(*SPLIT),) * 2, check_vma=False
    )
```

```python
import functools

import jax
import jax.numpy as jnp
import numpy as np
from jax import lax
from jax.experimental import pallas as pl
from jax.experimental.pallas import tpu as pltpu
from jax.sharding import PartitionSpec as P

SPLIT = ("tm", "lat", "lon")
tweedie_power = 1.6
smooth = 0.5

ROWS, LANES, SEG, LAT_OWN, LON_OWN, T_OWN = 80, 512, 40, 64, 32, 8
HOURS, LAT_CELLS, LON_CELLS = 32, 256, 128
EDGE, CHUNK = 16, 112
MID_CELLS, EDGE_CELLS = LAT_CELLS - 2 * EDGE, 2 * EDGE


def spline(offsets):
    distance = np.abs(offsets)
    near_part = (4.0 - 6.0 * distance**2 + 3.0 * distance**3) / 6.0
    far_part = np.maximum(2.0 - distance, 0.0) ** 3 / 6.0
    return np.where(distance < 1.0, near_part, far_part)


def table(cell_count, knot_count):
    cell_pos = np.arange(cell_count, dtype=np.float64)[:, None]
    knot_pos = np.arange(knot_count + 4, dtype=np.float64)[None, :] - 2.0
    return spline((cell_pos - 4.0 * knot_pos - 1.5) / 4.0)


def halves(values):
    values = jnp.asarray(values, jnp.float32)
    high = values.astype(jnp.bfloat16)
    return high, (values - high.astype(jnp.float32)).astype(jnp.bfloat16)


def middle(cells, axis=0):
    return lax.slice_in_dim(cells, EDGE, LAT_CELLS - EDGE, axis=axis)


def edges(cells, axis=0):
    ends = (lax.slice_in_dim(cells, at, at + EDGE, axis=axis) for at in (0, LAT_CELLS - EDGE))
    return jnp.concatenate(list(ends), axis=axis)


def tables():
    lat = np.zeros((LAT_CELLS, ROWS))
    lat[:, : LAT_OWN + 4] = table(LAT_CELLS, LAT_OWN)
    high, low = halves(lat)
    lat_tables = []
    for part in (middle, edges):
        up = jnp.concatenate([part(high), part(low), part(high)], axis=1)
        cells = CHUNK if part is middle else EDGE_CELLS
        down = [p.reshape(-1, cells, ROWS).transpose(0, 2, 1) for p in (part(high), part(low))]
        lat_tables += [up, jnp.concatenate([down[0], down[1], down[0]], axis=2)]
    lon = np.zeros((128, 3 * LON_CELLS))
    for r in range(3):
        lon[r * SEG : r * SEG + LON_OWN + 4, r * LON_CELLS : (r + 1) * LON_CELLS] = table(LON_CELLS, LON_OWN).T
    high, low = halves(lon)
    lon_up = jnp.concatenate([high, high, low], axis=0)
    lon_down = jnp.concatenate([high.T, low.T], axis=1)
    return lat_tables[:2] + [lon_up, lon_down], lat_tables[2:] + [lon_up, lon_down]


def hour_factors():
    near, far = ([float(spline(np.float64(x))) for x in xs] for xs in ((0.125, 0.875, 0.375, 0.625), (1.125, 1.875, 1.375, 1.625)))
    outer = ((far[0] + far[1]) / 2, (far[0] - far[1]) / 2, (far[2] + far[3]) / 2, (far[2] - far[3]) / 2)
    inner = ((near[0] + near[1]) / 2, (near[0] - near[1]) / 2, (near[2] + near[3]) / 2, (near[2] - near[3]) / 2)
    return outer, inner


class Place:
    def __init__(self):
        index = {axis: lax.axis_index(axis) for axis in SPLIT}
        self.even = {axis: index[axis] % 2 == 0 for axis in SPLIT}
        self.left = {axis: jnp.where(index[axis] > 0, 1.0, 0.0) for axis in SPLIT}
        self.right = {axis: jnp.where(index[axis] < lax.axis_size(axis) - 1, 1.0, 0.0) for axis in SPLIT}

    def messages(self, axis, to_left, to_right):
        return jnp.where(self.even[axis], to_left, to_right), jnp.where(self.even[axis], to_right, to_left)

    def received(self, axis, first, second):
        left, right = jnp.where(self.even[axis], first, second), jnp.where(self.even[axis], second, first)
        return (left, right) if axis == "lon" else (left * self.left[axis], right * self.right[axis])


def split(values):
    high = values.astype(jnp.bfloat16)
    return high, (values - high.astype(jnp.float32)).astype(jnp.bfloat16)


def dot(left, right):
    return jnp.dot(left, right, preferred_element_type=jnp.float32)


def lane_places():
    lane = lax.broadcasted_iota(jnp.int32, (ROWS, 128), 1)
    r = (lane >= SEG).astype(jnp.int32) + (lane >= 2 * SEG).astype(jnp.int32)
    return r, lane - SEG * r, lax.broadcasted_iota(jnp.int32, (ROWS, 128), 0)


def within(place, count):
    return (place >= 2) & (place < count + 2)


def group(values, g):
    return values[:, g * 128 : (g + 1) * 128]


def penalty(values, place):
    r, lon, row = lane_places()
    own_row, own_lon = within(row, LAT_OWN), within(lon, LON_OWN)
    row_share = jnp.where(
        own_row, 1.0, jnp.where(row == 1, 1.0 - place.left["lat"], jnp.where(row == LAT_OWN + 2, 1.0 - place.right["lat"], 0.0))
    )
    parts = [group(values, g) for g in range(4)]

    def along_t(v):
        before = [pltpu.roll(v[3], SEG, 1), v[0], v[1], v[2]]
        after = [v[1], v[2], v[3], pltpu.roll(v[0], 128 - SEG, 1)]
        return [b - 2.0 * m + a for b, m, a in zip(before, v, after)]

    t_second = along_t(parts)
    t_shared = []
    summed = []
    for g in range(4):
        t = 4 * r + g
        own_t = within(t, T_OWN)
        share = jnp.where(own_t, 1.0, jnp.where(t == 1, 1.0 - place.left["tm"], jnp.where(t == T_OWN + 2, 1.0 - place.right["tm"], 0.0)))
        t_shared.append(jnp.where(own_row & own_lon, share, 0.0) * t_second[g])
        v = parts[g]
        second = pltpu.roll(v, 1, 0) - 2.0 * v + pltpu.roll(v, ROWS - 1, 0)
        second = jnp.where(own_t & own_lon, row_share, 0.0) * second
        total = pltpu.roll(second, 1, 0) - 2.0 * second + pltpu.roll(second, ROWS - 1, 0)
        second = pltpu.roll(v, 1, 1) - 2.0 * v + pltpu.roll(v, 127, 1)
        second = jnp.where(own_t & own_lon & own_row, second, 0.0)
        summed.append(total + pltpu.roll(second, 1, 1) - 2.0 * second + pltpu.roll(second, 127, 1))
    return [smooth * (a + b) for a, b in zip(summed, along_t(t_shared))]


def lane_sum(parts):
    return jnp.sum(parts[0] + parts[1] + parts[2] + parts[3], axis=0, keepdims=True)


def own_lane_sum(values):
    r, lon, row = lane_places()
    inside = within(row, LAT_OWN) & within(lon, LON_OWN)
    return lane_sum([jnp.where(inside & within(4 * r + g, T_OWN), group(values, g), 0.0) for g in range(4)])


def merge_rows(values, got_first, got_second, place):
    keep = lax.broadcasted_iota(jnp.int32, (8, LANES), 0) < 4
    left, right = place.received("lat", got_first, got_second)
    return jnp.concatenate(
        [
            values[0:8] + jnp.where(keep, left, 0.0),
            values[8:64],
            values[64:72] + jnp.where(keep, right, 0.0),
            values[72:80],
        ],
        axis=0,
    )


def expand_cells(parts, lat_up, lon_up, up):
    expanded = dot(lat_up, parts)
    high, low = split(jnp.concatenate([group(expanded, g) for g in range(4)], axis=0))
    up[...] = dot(jnp.concatenate([high, low, high], axis=1), lon_up[...])


def cells_tile(w_of, first_row, start, cells, up, down):
    outer, inner = hour_factors()
    rows = pl.ds(first_row + start, 8)

    def knot(t):
        return up[pl.ds((t % 4) * cells + start, 8), (t // 4) * 128 : (t // 4 + 1) * 128]

    back = [None] * 12

    def add(t, value):
        back[t] = value if back[t] is None else back[t] + value

    x = [knot(0), knot(1), knot(2), None]
    for j in range(9):
        x[3] = knot(j + 3)
        edge_sum, edge_diff, mid_sum, mid_diff = x[0] + x[3], x[0] - x[3], x[1] + x[2], x[1] - x[2]
        sides = []
        for pair, (late, early) in enumerate(((2, 1), (3, 0))):
            even = outer[2 * pair] * edge_sum + inner[2 * pair] * mid_sum
            uneven = outer[2 * pair + 1] * edge_diff + inner[2 * pair + 1] * mid_diff
            below = w_of(4 * (j - 1) + late, rows, even + uneven) if j > 0 else None
            above = w_of(4 * j + early, rows, even - uneven) if j < 8 else None
            if below is None:
                sides.append((above, -above))
            elif above is None:
                sides.append((below, below))
            else:
                sides.append((below + above, below - above))
        (both0, differ0), (both1, differ1) = sides
        edge_even, edge_odd = outer[0] * both0 + outer[2] * both1, outer[1] * differ0 + outer[3] * differ1
        mid_even, mid_odd = inner[0] * both0 + inner[2] * both1, inner[1] * differ0 + inner[3] * differ1
        add(j, edge_even + edge_odd)
        add(j + 1, mid_even + mid_odd)
        add(j + 2, mid_even - mid_odd)
        add(j + 3, edge_even - edge_odd)
        for t in (j,) if j < 8 else (8, 9, 10, 11):
            down[pl.ds((t % 4) * cells + start, 8), (t // 4) * 128 : (t // 4 + 1) * 128] = back[t]
        x = [x[1], x[2], x[3], None]


def fold_cells(down, cells, lat_down, lon_down):
    high, low = split(down[...])
    both = dot(high, lon_down[...])
    narrow = both[:, :128] + both[:, 128:] + dot(low, lon_down[:, :128])
    narrow = jnp.concatenate([narrow[g * cells : (g + 1) * cells] for g in range(4)], axis=1)
    high, low = split(narrow)
    return dot(lat_down, jnp.concatenate([high, high, low], axis=0))


def apply_cells(values, w_of, lat_up, lat_down, lon_up, lon_down, *scratch):
    high, low = split(values)
    parts = jnp.concatenate([high, high, low], axis=0)
    chunks, _, _ = lat_down.shape
    cells = lat_up.shape[0] // chunks
    buffers = scratch[:2], scratch[2:]
    expand_cells(parts, lat_up[0:cells], lon_up, buffers[0][0])
    total = None
    for chunk in range(chunks):
        up, down = buffers[chunk % 2]
        if chunk + 1 < chunks:
            expand_cells(parts, lat_up[(chunk + 1) * cells : (chunk + 2) * cells], lon_up, buffers[(chunk + 1) % 2][0])
        for start in range(0, cells, 8):
            cells_tile(w_of, chunk * cells, start, cells, up, down)
        part = fold_cells(down, cells, lat_down[chunk], lon_down)
        total = part if total is None else total + part
    return total


def finish(total, values, place):
    extra = penalty(values, place)
    sums = [group(total, g) + extra[g] for g in range(4)]
    turned = [jnp.concatenate([part, jnp.zeros((128 - ROWS, 128), jnp.float32)], axis=0).T for part in sums]
    return sums, [[turned[g][r * SEG : (r + 1) * SEG] for g in range(4)] for r in range(3)]


def rolled(values, amount, axis):
    amount %= values.shape[axis]
    return pltpu.roll(values, amount, axis) if amount else values


def pack_lanes(parts):
    lane = lax.broadcasted_iota(jnp.int32, parts[0].shape, 1)
    rest = pltpu.roll(parts[0], 64, 1)
    for i in range(1, len(parts)):
        rest = jnp.where(lane < 4 * i, rest, pltpu.roll(parts[i], 64 + 4 * i, 1))
    pairs = [jnp.where(lane < 64, parts[i], pltpu.roll(parts[i + 1], 64, 1)) for i in range(0, len(parts), 2)]
    return pairs + [rest]


def unpack_lanes(packs, i):
    lane = lax.broadcasted_iota(jnp.int32, packs[0].shape, 1)
    main, rest = rolled(packs[i // 2], -64 * (i % 2), 1), rolled(packs[-1], 64 - 4 * i, 1)
    return jnp.where(lane < 64, main, jnp.where(lane < LAT_OWN + 4, rest, 0.0))


def write_ends(segs, place, tiles, first, second):
    lower = lax.broadcasted_iota(jnp.int32, (8, 128), 0) < 4
    sides = []
    for at in (0, 32):
        parts = []
        for r in range(3):
            for h in range(2):
                pair = (segs[r][2 * h + i][at : at + 8] for i in range(2))
                parts.append(jnp.where(lower, next(pair), pltpu.roll(next(pair), 4, 0)))
        sides.append(pack_lanes(parts))
    for r in range(3):
        for g in range(4):
            tiles[r, g] = segs[r][g]
    for i, pair in enumerate(zip(*sides)):
        first[i], second[i] = place.messages("lon", *pair)


def start_of(area, offset, precip, weight):
    def w_of(hour, rows, value):
        linear = offset[hour, rows, :] + value
        here = area[rows, :]
        w = here * jnp.exp((2.0 - tweedie_power) * linear)
        weight[hour, rows, :] = w
        return w - here * precip[hour, rows, :] * jnp.exp((1.0 - tweedie_power) * linear)

    return w_of


def load_kernel(_, offset_far, precip_far, offset, precip, offset_edges, precip_edges, arrived):
    copies = []

    def bring(source, source_at, target, target_at, count):
        source, target = source.at[:, pl.ds(source_at, count), :], target.at[:, pl.ds(target_at, count), :]
        copies.append(pltpu.make_async_copy(source, target, arrived.at[len(copies)]))

    for source, target, ends in ((offset_far, offset, offset_edges), (precip_far, precip, precip_edges)):
        bring(source, EDGE, target, 0, MID_CELLS)
        bring(source, 0, ends, 0, EDGE)
        bring(source, LAT_CELLS - EDGE, ends, EDGE, EDGE)
    for copy in copies:
        copy.start()
    for copy in copies:
        copy.wait()


def offset_kernel(_, area, offset, precip, rate, loss):
    def hour(h, carry):
        rate[h] = area[...] * jnp.exp((2.0 - tweedie_power) * offset[h])
        loss[h] = area[...] * precip[h] * jnp.exp((1.0 - tweedie_power) * offset[h])
        return carry

    lax.fori_loop(0, HOURS, hour, 0)


def start_middle_kernel(both, rate, loss, lat_up, lat_down, lon_up, lon_down, weight, total, *scratch):
    def w_of(hour, rows, value):
        w = rate[hour, rows, :] * jnp.exp((2.0 - tweedie_power) * value)
        weight[hour, rows, :] = w
        return w - loss[hour, rows, :] * jnp.exp((1.0 - tweedie_power) * value)

    total[...] = apply_cells(both[0], w_of, lat_up, lat_down, lon_up, lon_down, *scratch)


def start_kernel(both, got_first, got_second, total, area, offset, precip, lat_up, lat_down, lon_up, lon_down,
                 weight, diag, tiles, first, second, *scratch):
    place = Place()
    row = lax.broadcasted_iota(jnp.int32, (8, LANES), 0)
    left, right = place.received("lat", got_first[...], got_second[...])

    def with_halo(own, left, right):
        head, tail = own[0:8] + jnp.where(row < 2, left, 0.0), own[64:72] + jnp.where((row >= 2) & (row < 4), right, 0.0)
        return jnp.concatenate([head, own[8:64], tail, own[72:80]], axis=0)

    values = with_halo(both[0], left, right)
    diag[...] = with_halo(both[1], pltpu.roll(left, 6, 0), pltpu.roll(right, 6, 0))
    w_of = start_of(area, offset, precip, weight)
    part = apply_cells(values, w_of, lat_up, lat_down, lon_up, lon_down, *scratch)
    _, segs = finish(total[...] + part, values, place)
    write_ends(segs, place, tiles, first, second)


def weigh(weight):
    return lambda hour, rows, value: weight[hour, rows, :] * value


def hessian_middle_kernel(partial_rows, diag, weight, lat_up, lat_down, lon_up, lon_down, total, *scratch, again):
    here = partial_rows[...] if again else -partial_rows[...]
    total[...] = apply_cells(diag[...] * here, weigh(weight), lat_up, lat_down, lon_up, lon_down, *scratch)


def hessian_kernel(partial_rows, got_first, got_second, total, diag, weight, lat_up, lat_down, lon_up, lon_down, *refs, again):
    if again:
        before, residual, scaled, tiles, slots, *scratch = refs
    else:
        residual, scaled, tiles, first, second, sums, *scratch = refs
    place = Place()
    merged = merge_rows(partial_rows[...], got_first[...], got_second[...], place)
    here = merged if again else -merged
    residual[...] = here
    values = diag[...] * here
    scaled[...] = values
    part = apply_cells(values, weigh(weight), lat_up, lat_down, lon_up, lon_down, *scratch)
    image, segs = finish(total[...] + part, values, place)
    lines = [own_lane_sum(here * values), lane_sum([image[g] * group(values, g) for g in range(4)])]
    if again:
        for r in range(3):
            for g in range(4):
                tiles[r, g] = segs[r][g]
        lines = jnp.concatenate([jnp.zeros((4, 128), jnp.float32), before[0:2], *lines], axis=0)
        write_slots(image, segs, lines, slots)
    else:
        write_ends(segs, place, tiles, first, second)
        sums[...] = jnp.concatenate(lines + [jnp.zeros((6, 128), jnp.float32)], axis=0)


def slot_at(lon_step, lat_step):
    lon_count, lat_count = lax.axis_size("lon"), lax.axis_size("lat")
    lon = lax.rem(lax.axis_index("lon") + (lon_count + lon_step), lon_count)
    return lon * lat_count + lax.rem(lax.axis_index("lat") + (lat_count + lat_step), lat_count)


def row_of(shape=(8, 128)):
    return lax.broadcasted_iota(jnp.int32, shape, 0)


def write_slots(sums, segs, lines, slots):
    row = row_of()
    low = lax.broadcasted_iota(jnp.int32, (8, 128), 1) < LAT_OWN
    for j in range(slots.shape[0]):
        slots[j, 0:8] = jnp.zeros((8, 128), jnp.float32)
        slots[j, 8:16] = lines
    for step, at, skip in ((-1, 0, 0), (1, 32, 2)):
        halves_of = [jnp.zeros((8, 128), jnp.float32), lines]
        for r in range(3):
            for h in range(2):
                index = 2 * r + h
                pair = jnp.where(
                    low, pltpu.roll(segs[r][2 * h][at : at + 8], 126, 1), pltpu.roll(segs[r][2 * h + 1][at : at + 8], 62, 1)
                )
                to = 2 * (index % 4)
                part = rolled(pair, to - skip, 0)
                halves_of[index // 4] = jnp.where((row >= to) & (row < to + 2), part, halves_of[index // 4])
        slot = slot_at(step, 0)
        slots[slot, 0:8] = halves_of[0]
        slots[slot, 8:16] = halves_of[1]
    for lat_step, at, skip in ((-1, 0, 0), (1, 64, 2)):
        content = jnp.zeros((8, 128), jnp.float32)
        for g in range(4):
            part = rolled(sums[g][at : at + 8], 2 * g - skip, 0)
            content = jnp.where((row >= 2 * g) & (row < 2 * g + 2), part, content)
        for lon_step in (-1, 0, 1):
            slots[slot_at(lon_step, lat_step), 0:8] = content


def collect_kernel(tiles, slots, merged, first, second, lines):
    place = Place()
    row = row_of()
    lane = lax.broadcasted_iota(jnp.int32, (8, 128), 1)
    own_lane = within(lane, LAT_OWN)
    r_of = (lane >= SEG).astype(jnp.int32) + (lane >= 2 * SEG).astype(jnp.int32)
    lon = lane - SEG * r_of
    sides = []
    for lat_step, share in ((-1, place.left["lat"]), (1, place.right["lat"])):
        before, same, after = (slots[slot_at(lon_step, lat_step), 0:8] for lon_step in (-1, 0, 1))
        side = jnp.where(within(lon, LON_OWN), same, 0.0)
        side = side + jnp.where(within(lon, 2), pltpu.roll(before, 128 - LON_OWN, 1), 0.0)
        side = side + jnp.where((lon >= LON_OWN) & (lon < LON_OWN + 2), pltpu.roll(after, LON_OWN, 1), 0.0)
        sides.append(side * share)
    blank = jnp.zeros((56, 128), jnp.float32)
    from_lat = []
    for g in range(4):
        head = jnp.where(within(row, 2), rolled(sides[0], 2 - 2 * g, 0), 0.0)
        tail = jnp.where(row < 2, rolled(sides[1], -2 * g, 0), 0.0)
        from_lat.append(jnp.concatenate([head, blank, tail, blank], axis=0).T)
    left = [slots[slot_at(-1, 0), at : at + 8] for at in (0, 8)]
    right = [slots[slot_at(1, 0), at : at + 8] for at in (0, 8)]
    for r in range(3):
        for g in range(4):
            index = 2 * r + g // 2
            shift = 66 if g % 2 else 2
            to = 2 * (index % 4)
            head = jnp.where(within(row, 2) & own_lane, pltpu.roll(rolled(left[index // 4], 2 - to, 0), shift, 1), 0.0)
            tail = jnp.where((row < 2) & own_lane, pltpu.roll(rolled(right[index // 4], -to, 0), shift, 1), 0.0)
            seg = tiles[r, g] + from_lat[g][r * SEG : (r + 1) * SEG]
            merged[r, g] = jnp.concatenate([seg[0:8] + head, seg[8:32], seg[32:40] + tail], axis=0)
    total = slots[0, 8:16]
    for j in range(1, slots.shape[0]):
        total = total + slots[j, 8:16]
    lines[...] = total
    low = lax.broadcasted_iota(jnp.int32, (SEG, 128), 1) < LAT_OWN

    def message(r, g):
        data = jnp.where(low, pltpu.roll(merged[r, g], 126, 1), pltpu.roll(merged[r, g + 1], 62, 1))
        return jnp.concatenate([data[:32], jnp.where(row < 4, data[32:], total)], axis=0)

    first[...], second[...] = place.messages("tm", message(0, 0), message(2, 2))


def join_kernel(tiles, got_first, got_second, joined, first, second):
    place = Place()
    lower = lax.broadcasted_iota(jnp.int32, (8, 128), 0) < 4
    lefts, rights = zip(*(place.received("lon", got_first[i], got_second[i]) for i in range(4)))
    for r in range(3):
        for h in range(2):
            pair_left, pair_right = unpack_lanes(lefts, 2 * r + h), unpack_lanes(rights, 2 * r + h)
            for g in (2 * h, 2 * h + 1):
                left, right = rolled(pair_left, 4 * (g % 2), 0), rolled(pair_right, 4 * (g % 2), 0)
                joined[r, g, 0:8] = tiles[r, g, 0:8] + jnp.where(lower, left, 0.0)
                joined[r, g, 8:32] = tiles[r, g, 8:32]
                joined[r, g, 32:40] = tiles[r, g, 32:40] + jnp.where(lower, right, 0.0)
    for i, pair in enumerate(zip(*(pack_lanes([joined[r, g] for g in range(4)]) for r in (0, 2)))):
        first[i], second[i] = place.messages("tm", *pair)


def turned_rows(tiles, g, left=0.0, right=0.0):
    parts = [tiles[0, g] + left, tiles[1, g], tiles[2, g] + right, jnp.zeros((8, 128), jnp.float32)]
    return jnp.concatenate(parts, axis=0).T


def turn_kernel(tiles, got_first, got_second, rows, first, second):
    place = Place()
    lefts, rights = zip(*(place.received("tm", got_first[i], got_second[i]) for i in range(3)))
    for g in range(4):
        block = turned_rows(tiles, g, unpack_lanes(lefts, g), unpack_lanes(rights, g))
        lanes = slice(g * 128, (g + 1) * 128)
        rows[:, lanes] = block[:ROWS]
        first[:, lanes], second[:, lanes] = place.messages("lat", block[0:8], block[64:72])


def embed_kernel(own_both, tiles, first, second):
    place = Place()
    pair = lax.broadcasted_iota(jnp.int32, (8, 128), 0) // 2
    heads, tails = [None] * 4, [None] * 4
    for t in range(12):
        for k in range(2):
            if 2 <= t < T_OWN + 2:
                own = jnp.concatenate([own_both[k, t - 2], jnp.zeros((LON_OWN, 128 - LAT_OWN), jnp.float32)], axis=1)
                own = jnp.concatenate([own, jnp.zeros((SEG - LON_OWN, 128), jnp.float32)], axis=0)
                seg = pltpu.roll(pltpu.roll(own, 2, 0), 2, 1)
                at, tile = 2 * (t % 2) + k, (t - 2) // 2
                head, tail = rolled(seg[0:8], 2 * at - 2, 0), rolled(seg[32:40], 2 * at, 0)
                heads[tile] = head if at == 0 else jnp.where(pair == at, head, heads[tile])
                tails[tile] = tail if at == 0 else jnp.where(pair == at, tail, tails[tile])
            else:
                seg = jnp.zeros((SEG, 128), jnp.float32)
            tiles[k, t // 4, t % 4] = seg
    for tile in range(4):
        first[tile], second[tile] = place.messages("lon", heads[tile], tails[tile])


def embed_join_kernel(tiles, got_first, got_second, _, joined, first, second):
    place = Place()
    row = lax.broadcasted_iota(jnp.int32, (8, 128), 0)
    for k in range(2):
        for t in range(12):
            r, g = t // 4, t % 4
            if 2 <= t < T_OWN + 2:
                at, tile = 2 * (t % 2) + k, (t - 2) // 2
                left, right = place.received("lon", got_first[tile], got_second[tile])
                left, right = rolled(left, -2 * at, 0), rolled(right, 2 - 2 * at, 0)
                joined[k, r, g, 0:8] = tiles[k, r, g, 0:8] + jnp.where(row < 2, left, 0.0)
                joined[k, r, g, 8:32] = tiles[k, r, g, 8:32]
                joined[k, r, g, 32:40] = tiles[k, r, g, 32:40] + jnp.where((row >= 2) & (row < 4), right, 0.0)
            else:
                joined[k, r, g] = tiles[k, r, g]
    low = lax.broadcasted_iota(jnp.int32, (SEG, 128), 1) < LAT_OWN

    def beside(r, g):
        return jnp.where(low, pltpu.roll(joined[0, r, g], 126, 1), pltpu.roll(joined[1, r, g], 62, 1))

    for i in range(2):
        first[i], second[i] = place.messages("tm", beside(0, 2 + i), beside(2, i))


def embed_turn_kernel(tiles, got_first, got_second, _, rows, first, second):
    place = Place()
    lane = lax.broadcasted_iota(jnp.int32, (SEG, 128), 1)
    own = (lane >= 2) & (lane < LAT_OWN + 2)
    row = lax.broadcasted_iota(jnp.int32, (8, 128), 0)
    for g in range(4):
        lanes = slice(g * 128, (g + 1) * 128)
        left, right = place.received("tm", got_first[g % 2], got_second[g % 2])
        blocks = []
        for k in range(2):
            shift = 66 if k else 2
            if g < 2:
                block = turned_rows(tiles.at[k], g, left=jnp.where(own, pltpu.roll(left, shift, 1), 0.0))
            else:
                block = turned_rows(tiles.at[k], g, right=jnp.where(own, pltpu.roll(right, shift, 1), 0.0))
            rows[k, :, lanes] = block[:ROWS]
            blocks.append(block)
        head = jnp.where(row < 4, blocks[0][0:8], pltpu.roll(blocks[1][0:8], 2, 0))
        tail = jnp.where(row < 2, blocks[0][64:72], pltpu.roll(blocks[1][64:72], 2, 0))
        first[:, lanes], second[:, lanes] = place.messages("lat", head, tail)


def ready_kernel(_, *refs):
    for source, target in zip(refs[:4], refs[4:]):
        for g in range(4):
            turned = jnp.concatenate([source[:, g * 128 : (g + 1) * 128], jnp.zeros((128 - ROWS, 128), jnp.float32)], axis=0).T
            turned = pltpu.roll(turned, 126, 1)
            for r in range(3):
                t = 4 * r + g - 2
                if 0 <= t < T_OWN:
                    target[t] = pltpu.roll(turned[r * SEG : (r + 1) * SEG], SEG - 2, 0)[:LON_OWN]


def last_kernel(tiles, got_first, got_second, lines, got_lines, residual, scaled, image, image_scaled, step_out, residual_out):
    place = Place()
    total = lines[...] + got_lines[...] + got_first[32:40] + got_second[32:40]
    norms, curvatures, image_norms, image_curvatures = (total[i : i + 1] for i in range(4, 8))

    def all_lanes(values):
        return jnp.sum(values, axis=1, keepdims=True)

    norm = all_lanes(norms)
    step_size = norm / all_lanes(curvatures)
    next_norm = all_lanes(norms + step_size * (step_size * image_norms - 2.0 * curvatures))
    next_curvature = all_lanes(curvatures + step_size * (step_size * image_curvatures - 2.0 * image_norms))
    ratio = next_norm / norm
    step_next = next_norm / (next_curvature - ratio * next_norm / step_size)
    left, right = place.received("tm", got_first[...], got_second[...])
    for t in range(T_OWN):
        merged = pltpu.roll(tiles[(t + 2) // 4, (t + 2) % 4], 126, 1)
        if t in (0, 1, T_OWN - 2, T_OWN - 1):
            merged = merged + rolled(left if t < 2 else right, 64 * (t % 2), 1)
        merged = pltpu.roll(merged, SEG - 2, 0)[:LON_OWN]
        s, y = scaled[t], image[t]
        step_out[t] = (step_size * s + step_next * (s - step_size * image_scaled[t] + ratio * s))[:, :LAT_OWN]
        left_over = residual[t] - step_size * y - step_next * (y - step_size * merged + ratio * y)
        residual_out[t] = left_over[:, :LAT_OWN]


def matchings(count):
    return [(i, (((i + 1) ^ 1) - 1) % count) for i in range(count)], [(i, i ^ 1) for i in range(count)]


def swap(first, second, axis):
    first_pairs, second_pairs = matchings(lax.axis_size(axis))
    return lax.ppermute(first, axis, first_pairs), lax.ppermute(second, axis, second_pairs)


def shaped(*shape):
    return jax.ShapeDtypeStruct(shape, jnp.float32)


def call(kernel, out_shape, name, *args, scratch=(), far=(), limit=24):
    vmem = pl.BlockSpec(memory_space=pltpu.VMEM)
    hbm = pl.BlockSpec(memory_space=pltpu.HBM)
    return pl.pallas_call(
        kernel,
        in_specs=[hbm if i in far else vmem for i in range(len(args))],
        out_specs=[vmem] * len(out_shape),
        out_shape=out_shape,
        scratch_shapes=scratch,
        compiler_params=pltpu.CompilerParams(vmem_limit_bytes=int(limit * 1024) * 1024),
        cost_estimate=pl.CostEstimate(flops=10**9, bytes_accessed=20 * 10**6, transcendentals=0),
        name=name,
    )(*args)


LON_MESSAGE, TM_MESSAGE, LAT_MESSAGE = (4, 8, 128), (3, SEG, 128), (8, LANES)
TILES = (3, 4, SEG, 128)
VECTOR = (ROWS, LANES)
MID_SCRATCH, EDGE_SCRATCH = ([pltpu.VMEM((4 * n, 384), jnp.float32)] * m for n, m in ((CHUNK, 4), (EDGE_CELLS, 2)))
LOAD_LIMIT = 42
MID, ENDS = ((HOURS, n, LON_CELLS) for n in (MID_CELLS, EDGE_CELLS))


def exchange(tiles, first, second):
    first, second = swap(first, second, "lon")
    tiles, first, second = call(
        join_kernel, (shaped(*TILES), shaped(*TM_MESSAGE), shaped(*TM_MESSAGE)), "join", tiles, first, second
    )
    first, second = swap(first, second, "tm")
    rows, first, second = call(
        turn_kernel, (shaped(*VECTOR), shaped(*LAT_MESSAGE), shaped(*LAT_MESSAGE)), "turn", tiles, first, second
    )
    return rows, *swap(first, second, "lat")


def fold_and_sum(tiles, slots, lines_shape):
    slots = lax.all_to_all(slots, ("lon", "lat"), 0, 0, tiled=True)
    message = shaped(SEG, 128)
    tiles, first, second, lines = call(
        collect_kernel, (shaped(*TILES), message, message, lines_shape), "collect", tiles, slots
    )
    first, second = swap(first, second, "tm")
    count = lax.axis_size("tm")
    got_lines = lax.ppermute(lines, "tm", [(i, (i + 2) % count) for i in range(count)])
    return tiles, first, second, lines, got_lines


def expand(coefficients, inverse_diag, offset, precip, area):
    tiles, message = shaped(2, *TILES), shaped(4, 8, 128)
    tiles_here, first, second = call(
        embed_kernel, (tiles, message, message), "embed", jnp.stack([coefficients, inverse_diag])
    )
    cells = call(
        load_kernel, (shaped(*MID), shaped(*MID), shaped(*ENDS), shaped(*ENDS)), "load", first, offset, precip,
        scratch=[pltpu.SemaphoreType.DMA((6,))], far=(1, 2), limit=LOAD_LIMIT,
    )
    first, second = swap(first, second, "lon")
    message = shaped(2, SEG, 128)
    tiles_here, first, second = call(embed_join_kernel, (tiles, message, message), "embed_join", tiles_here, first, second, cells[2])
    shares = call(offset_kernel, (shaped(*MID), shaped(*MID)), "offset", first, middle(area), *cells[:2])
    first, second = swap(first, second, "tm")
    shapes = (shaped(2, *VECTOR), shaped(*LAT_MESSAGE), shaped(*LAT_MESSAGE))
    both, first, second = call(embed_turn_kernel, shapes, "embed_turn", tiles_here, first, second, shares[0])
    return both, *swap(first, second, "lat"), cells, shares


def per_device(precip, offset, coefficients, inverse_diag):
    lat_total = LAT_CELLS * lax.axis_size("lat")
    lat_index = (lax.axis_index("lat") * LAT_CELLS + jnp.arange(LAT_CELLS, dtype=jnp.int32)).astype(jnp.float32)
    area = jnp.cos((90.0 - (lat_index + 0.5) * 180.0 / lat_total) * (jnp.pi / 180.0))
    area = jnp.broadcast_to(area[:, None], (LAT_CELLS, LON_CELLS))
    mid_tabs, edge_tabs = tables()
    ends = (shaped(*TILES), shaped(*LON_MESSAGE), shaped(*LON_MESSAGE))
    vector = shaped(*VECTOR)

    both, *got, cells, shares = expand(coefficients.transpose(0, 2, 1), inverse_diag.transpose(0, 2, 1), offset, precip, area)
    weight, total = call(
        start_middle_kernel, (shaped(*MID), vector), "start_middle", both, *shares, *mid_tabs, scratch=MID_SCRATCH
    )
    edge_weight, diag, *sent = call(
        start_kernel, (shaped(*ENDS), vector, *ends), "start", both, *got, total, edges(area), *cells[2:],
        *edge_tabs, scratch=EDGE_SCRATCH,
    )

    def hessian(again, rows, got, outs, *more):
        total, = call(
            functools.partial(hessian_middle_kernel, again=again), (vector,), "hessian_middle", rows, diag, weight, *mid_tabs,
            scratch=MID_SCRATCH,
        )
        return call(
            functools.partial(hessian_kernel, again=again), (vector, vector, *outs), "hessian", rows, *got, total, diag,
            edge_weight, *edge_tabs, *more, scratch=EDGE_SCRATCH,
        )

    lines = shaped(8, 128)
    rows, *got = exchange(*sent)
    residual, scaled, *sent, sums = hessian(False, rows, got, (*ends, lines))
    slots = shaped(lax.axis_size("lon") * lax.axis_size("lat"), 16, 128)
    rows, *got = exchange(*sent)
    image, image_scaled, tiles, slots = hessian(True, rows, got, (ends[0], slots), sums)
    out = shaped(T_OWN, LON_OWN, LAT_OWN)
    folded = fold_and_sum(tiles, slots, lines)
    ready = call(
        ready_kernel, (shaped(T_OWN, LON_OWN, 128),) * 4, "ready", folded[3], residual, scaled, image, image_scaled
    )
    outs = call(last_kernel, (out, out), "last", *folded, *ready)
    return tuple(v.transpose(0, 2, 1) for v in outs)


def solution(mesh):
    return jax.shard_map(
        per_device, mesh=mesh, in_specs=(P(*SPLIT),) * 4, out_specs=(P(*SPLIT),) * 2, check_vma=False
    )
```
